32 devices in a mesh: groups: 2 (over y), seq: 4 (over z), head: 4 (over x, core).
Axes of the slice: x: 2, y: 2, z: 4, core: 2. Of those that a mesh axis runs over, the one named last changes fastest.
Arguments:
- tile_rows: bfloat16 [8192, 1536], P(('groups', 'seq', 'head')), parts along dimension 0, may hold values from -6 to 6
- tile_route: int32 [8192, 2], P(('groups', 'seq', 'head')), parts along dimension 0, may hold values from 0 to 255, as said below
- embed_weight: bfloat16 [1536, 768], replicated, may hold values from -0.15625 to 0.15625
- norm_gain: float32 [768], replicated, may hold values from 0.1 to 1.9
- qkv_weight: bfloat16 [768, 16, 3, 48], P(None, 'head'), may hold values from -1 to 1
- out_weight: bfloat16 [768, 768], P('head'), may hold values from -0.21875 to 0.21875
Outputs:
- mixed: bfloat16 [8192, 768], P(('groups', 'seq', 'head')), parts along dimension 0
The draws below stay inside these ranges and needn't reach their ends.
There are 2 independent parts, one for each index of `groups`. The reference program is written for one: setup_inputs(seed, part) draws one part's arguments, and reference() takes and returns one part's arrays. A program takes and returns all parts, laid end to end along the dimension named above; an argument that names none is the same for every part. Nothing has to cross between parts.
Inputs may be any that keep to these rules, and one draw needn't show every extreme that they name: `tile_route`: A tile's owner holds the same head class as the tile's own device. From one device at most 128 tiles go to one index of seq, and some device sends exactly 128 to one index in every draw; every slot of every owner receives exactly one tile.
All inputs are finite; a program needn't handle non-finite values.
Results may differ from the reference program's by a relative error of at most 0.0075.
Values may be sent and summed in bfloat16 or wider, within the bound.
No kernel may reach another device: no remote copies, remote signals or barrier semaphores. Data moves between devices by JAX's collectives and lax.ppermute only.
A program may use at most 64 MiB of HBM per device.

```python
import jax
import jax.numpy as jnp
from jax import lax

D_IN = 1536
D = 768
HEADS = 16
HEAD_DIM = 48
TILES_DEV = 1024
TILES = 4096
IN_DEV = 256
CAP = 128
N_SEQ = 4
N_HEAD = 4


def route_table(key):
    count_seq = N_SEQ
    per_device = IN_DEV
    capacity = CAP
    shift_count = count_seq // 2 + 1

    def one_class(class_key):
        key_shift, key_split, key_source, key_target = jax.random.split(class_key, 4)
        shifts = jax.random.permutation(key_shift, count_seq)[:shift_count].astype(jnp.int32)
        extra = jax.random.randint(key_split, (), 1, capacity).astype(jnp.int32)
        loads = jnp.concatenate([jnp.full((shift_count - 2,), capacity, jnp.int32), jnp.stack([extra, capacity - extra])])
        ends = jnp.cumsum(loads)
        places = jnp.arange(per_device, dtype=jnp.int32)
        block = jnp.sum((places[:, None] >= ends[None, :]).astype(jnp.int32), axis=1)
        source_keys = jax.random.split(key_source, count_seq)
        order = jax.vmap(lambda sub: jax.random.permutation(sub, per_device))(source_keys).astype(jnp.int32)
        target_keys = jax.random.split(key_target, count_seq)
        slot_perm = jax.vmap(lambda sub: jax.random.permutation(sub, per_device))(target_keys).astype(jnp.int32)
        sources = jnp.arange(count_seq, dtype=jnp.int32)[:, None]
        owner = (sources + shifts[block[order]]) % count_seq
        slot_index = slot_perm[owner, order]
        return (owner, slot_index)
    class_keys = jax.random.split(key, N_HEAD)
    owner, slot_index = jax.vmap(one_class)(class_keys)
    owner = jnp.transpose(owner, (1, 0, 2)).reshape(-1)
    slot_index = jnp.transpose(slot_index, (1, 0, 2)).reshape(-1)
    return jnp.stack([owner, slot_index], axis=1).astype(jnp.int32)


def draw_tile_route(key, part):
    return route_table(jax.random.fold_in(key, 11))


def draw_qkv_weight(key, part):
    key_base = jax.random.fold_in(jax.random.fold_in(key, 23), 0)
    base = jax.random.normal(key_base, (D, HEADS, 3, HEAD_DIM), jnp.float32)
    weight = base * (1.5 * D ** (-0.5))
    return jnp.clip(weight, -1.0, 1.0).astype(jnp.bfloat16)


def levels(own_key, shape, shards, low, high):
    level = 1.0
    for dim, shards_of in shards:
        steps = jax.random.uniform(jax.random.fold_in(jax.random.fold_in(own_key, 6), dim), (shards_of,), jnp.float32, low / len(shards), high / len(shards))
        level = level * jnp.repeat(jnp.exp(steps), shape[dim] // shards_of).reshape((-1,) + (1,) * (len(shape) - 1 - dim))
    return level


def normal_values(own_key, extent, deviation, limit, shards=(), kind=jnp.bfloat16):
    values = deviation * jax.random.normal(own_key, extent, jnp.float32)
    if shards:
        values = values * levels(own_key, extent, shards, -0.22, 0.18)
    return jnp.clip(values, -limit, limit).astype(kind)


def setup_inputs(seed: int = 0, part: int = 0) -> dict:
    key_of = jax.random.split(jax.random.key(seed), 7)
    part_keys = jax.random.split(jax.random.fold_in(key_of[6], part), 7)
    return {
        "tile_rows": normal_values(part_keys[0], (TILES, D_IN), 1.0, 6.0, ((0, 16),)),
        "tile_route": draw_tile_route(jax.random.fold_in(jax.random.fold_in(key_of[6], part), 71), part),
        "embed_weight": normal_values(key_of[2], (D_IN, D), D_IN ** -0.5, 0.15625),
        "norm_gain": jnp.clip(1.0 + 0.18 * jax.random.normal(key_of[3], (D,), jnp.float32), 0.1, 1.9),
        "qkv_weight": draw_qkv_weight(jax.random.fold_in(key_of[6], 71), part),
        "out_weight": normal_values(key_of[5], (D, D), D ** -0.5, 0.21875, ((0, 4),)),
    }


EPSILON = 1e-05
DILATIONS = (1, 4, 16)
FRACTIONS = (16, 4, 1)

def layer_norm(rows, gain):
    rows = rows.astype(jnp.float32)
    row_mean = lax.optimization_barrier(jnp.mean(rows, axis=-1, keepdims=True))
    centered = rows - row_mean
    row_var = lax.optimization_barrier(jnp.mean(centered * centered, axis=-1, keepdims=True))
    return (centered * lax.rsqrt(row_var + EPSILON) * gain.astype(jnp.float32)).astype(jnp.bfloat16)

def attend_block(queries, key_rows, values):
    score_scale = queries.shape[-1] ** (-0.5)
    scores = jnp.dot(queries, key_rows.T, preferred_element_type=jnp.float32) * score_scale
    row_max = lax.optimization_barrier(jnp.max(scores, axis=-1))
    expo = jnp.exp(scores - row_max[:, None])
    denominator = lax.optimization_barrier(jnp.sum(expo, axis=-1))
    weights = (expo / denominator[:, None]).astype(jnp.bfloat16)
    head_out = jnp.dot(weights, values, preferred_element_type=jnp.float32)
    return (head_out, row_max + jnp.log(denominator))

def expand_rows(head_out, log_total, offset, dilation):
    count = head_out.shape[0]
    pick_mask = jnp.arange(dilation, dtype=jnp.int32) == offset
    full_out = jnp.where(pick_mask[None, :, None], head_out[:, None, :], 0.0).reshape(count * dilation, -1)
    full_total = jnp.where(pick_mask[None, :], log_total[:, None], -1e+30).reshape(count * dilation)
    return (full_out, full_total)

def merge_scales(outputs, totals):
    row_max = jnp.maximum(jnp.maximum(totals[0], totals[1]), totals[2])
    numer = jnp.zeros_like(outputs[0])
    denom = jnp.zeros_like(totals[0])
    for full_out, full_total in zip(outputs, totals):
        factor = jnp.exp(full_total - row_max)
        numer = numer + factor[:, None] * full_out
        denom = denom + factor
    return numer / denom[:, None]

def one_head(head_index, qkv_head):
    outputs = []
    totals = []
    head_dim = qkv_head.shape[-1]
    for fraction, dilation in zip(FRACTIONS, DILATIONS):
        segment = TILES // fraction
        offset = (head_index % dilation).astype(jnp.int32)
        shaped = qkv_head.reshape(TILES // dilation, dilation, 3, head_dim)
        picked = lax.dynamic_index_in_dim(shaped, offset, axis=1, keepdims=False)
        grouped = picked.reshape(TILES // segment, segment // dilation, 3, head_dim)
        head_out, log_total = lax.map(lambda block_in: attend_block(block_in[:, 0], block_in[:, 1], block_in[:, 2]), grouped)
        full_out, full_total = expand_rows(head_out.reshape(TILES // dilation, head_dim), log_total.reshape(TILES // dilation), offset, dilation)
        outputs.append(full_out)
        totals.append(full_total)
    return merge_scales(outputs, totals).astype(jnp.bfloat16)

def reference(tile_rows, tile_route, embed_weight, norm_gain, qkv_weight, out_weight):
    projected = jnp.dot(tile_rows, embed_weight, preferred_element_type=jnp.float32).astype(jnp.bfloat16)
    position = jnp.arange(TILES, dtype=jnp.int32)
    head_class = position // IN_DEV % N_HEAD
    target = tile_route[:, 0] * TILES_DEV + head_class * IN_DEV + tile_route[:, 1]
    embedded = jnp.zeros((TILES, D), jnp.bfloat16).at[target].set(projected)
    normed = layer_norm(embedded, norm_gain)
    qkv = jnp.dot(normed, qkv_weight.reshape(D, -1), preferred_element_type=jnp.float32).astype(jnp.bfloat16)
    qkv = qkv.reshape(TILES, HEADS, 3, HEAD_DIM).transpose(1, 0, 2, 3)
    heads_out = lax.map(lambda pair: one_head(pair[0], pair[1]), (jnp.arange(HEADS, dtype=jnp.int32), qkv))
    attention = heads_out.transpose(1, 0, 2).reshape(TILES, D)
    mixed = embedded.astype(jnp.float32) + jnp.dot(attention, out_weight, preferred_element_type=jnp.float32)
    return mixed.astype(jnp.bfloat16)
```

```python
import functools

import jax
import jax.numpy as jnp
from jax import lax
from jax.experimental import pallas as pl
from jax.experimental.pallas import tpu as pltpu
from jax.sharding import PartitionSpec as P

EPSILON = 1e-05
DILATIONS = (1, 4, 16)
FRACTIONS = (16, 4, 1)


def from_partner(block, axis, apart):
    count = lax.axis_size(axis)
    route = []
    for low in range(count):
        high = low | 1 << apart
        if high != low and high < count:
            route += [(low, high), (high, low)]
    return lax.ppermute(block, axis, route)


def layer_norm(rows, gain):
    row_mean = jnp.mean(rows, axis=-1, keepdims=True)
    centered = rows - row_mean
    row_var = jnp.mean(centered * centered, axis=-1, keepdims=True)
    return (centered * lax.rsqrt(row_var + EPSILON) * gain).astype(jnp.bfloat16)


def attend_block(queries, key_rows, values):
    score_scale = queries.shape[-1] ** (-0.5)
    scores = jnp.dot(queries, key_rows.T, preferred_element_type=jnp.float32) * score_scale
    row_max = jnp.max(scores, axis=-1)
    expo = jnp.exp(scores - row_max[:, None])
    denominator = jnp.sum(expo, axis=-1)
    weights = (expo / denominator[:, None]).astype(jnp.bfloat16)
    head_out = jnp.dot(weights, values, preferred_element_type=jnp.float32)
    return (head_out, row_max + jnp.log(denominator))


def attend(queries, key_rows, values):
    count = queries.shape[0]
    if count > 512 and count % 512 == 0:
        blocks = queries.reshape(count // 512, 512, queries.shape[1])
        head_out, log_total = lax.map(
            lambda block_in: attend_block(block_in, key_rows, values), blocks
        )
        return (head_out.reshape(count, -1), log_total.reshape(count))
    return attend_block(queries, key_rows, values)


def expand_rows(head_out, log_total, offset, dilation):
    count = head_out.shape[0]
    pick_mask = jnp.arange(dilation, dtype=jnp.int32) == offset
    full_out = jnp.where(pick_mask[None, :, None], head_out[:, None, :], 0.0).reshape(
        count * dilation, -1
    )
    full_total = jnp.where(pick_mask[None, :], log_total[:, None], -1e30).reshape(count * dilation)
    return (full_out, full_total)


def merge_scales(outputs, totals):
    row_max = jnp.maximum(jnp.maximum(totals[0], totals[1]), totals[2])
    numer = jnp.zeros_like(outputs[0])
    denom = jnp.zeros_like(totals[0])
    for full_out, full_total in zip(outputs, totals):
        factor = jnp.exp(full_total - row_max)
        numer = numer + factor[:, None] * full_out
        denom = denom + factor
    return numer / denom[:, None]


def collect_segment(flat_rows, levels, seq_index):
    for level in range(levels):
        partner = from_partner(flat_rows, "seq", level)
        upper_half = seq_index >> level & 1 == 1
        lower_rows = jnp.where(upper_half, partner, flat_rows)
        upper_rows = jnp.where(upper_half, flat_rows, partner)
        flat_rows = jnp.concatenate([lower_rows, upper_rows], axis=0)
    return flat_rows


def general(tile_rows, tile_route, embed_weight, norm_gain, qkv_weight, out_weight):
    seq_count = lax.axis_size("seq")
    seq_index = lax.axis_index("seq")
    in_rows = tile_rows.shape[0]
    width = embed_weight.shape[1]
    capacity = 2 * in_rows // seq_count
    projected = jnp.dot(tile_rows, embed_weight, preferred_element_type=jnp.float32).astype(
        jnp.bfloat16
    )
    dest_seq = tile_route[:, 0]
    slot_index = tile_route[:, 1]
    owner_hits = (dest_seq[:, None] == jnp.arange(seq_count, dtype=jnp.int32)[None, :]).astype(
        jnp.int32
    )
    earlier = jnp.cumsum(owner_hits, axis=0) - owner_hits
    owner_rank = jnp.sum(earlier * owner_hits, axis=1)
    buffer_place = dest_seq * capacity + owner_rank
    send_pick = jnp.arange(seq_count * capacity, dtype=jnp.int32)[:, None] == buffer_place[None, :]
    outgoing = jnp.dot(
        send_pick.astype(jnp.bfloat16), projected, preferred_element_type=jnp.float32
    ).astype(jnp.bfloat16)
    outgoing_slot = jnp.sum(jnp.where(send_pick, slot_index[None, :] + 1, 0), axis=1)
    arrived, arrived_slot = (
        lax.all_to_all(
            outgoing.reshape(seq_count, capacity, width),
            "seq",
            split_axis=0,
            concat_axis=0,
            tiled=True,
        ),
        lax.all_to_all(
            outgoing_slot.reshape(seq_count, capacity),
            "seq",
            split_axis=0,
            concat_axis=0,
            tiled=True,
        ),
    )
    landing = jnp.arange(in_rows, dtype=jnp.int32)[:, None] + 1 == arrived_slot.reshape(-1)[None, :]
    embedded = jnp.dot(
        landing.astype(jnp.bfloat16), arrived.reshape(-1, width), preferred_element_type=jnp.float32
    )
    normed = layer_norm(embedded, norm_gain)
    heads_here = qkv_weight.shape[1]
    head_dim = qkv_weight.shape[3]
    weight_flat = qkv_weight.reshape(width, -1)
    qkv = jnp.dot(
        lax.all_gather(normed, "head", axis=0, tiled=True),
        weight_flat,
        preferred_element_type=jnp.float32,
    ).astype(jnp.bfloat16)
    rows_here = qkv.shape[0]
    qkv = qkv.reshape(rows_here, heads_here, 3, head_dim)
    first_head = lax.axis_index("head") * heads_here
    total_rows = rows_here * seq_count
    outputs = [[] for member in range(heads_here)]
    totals = [[] for member in range(heads_here)]
    for fraction, dilation in zip(FRACTIONS, DILATIONS):
        segment = total_rows // fraction
        per_segment = segment // dilation
        count = rows_here // dilation
        shaped = qkv.reshape(count, dilation, heads_here, 3, head_dim)
        offsets = []
        chosen = []
        for member in range(heads_here):
            offset = (first_head + member) % dilation
            offsets.append(offset)
            chosen.append(
                lax.dynamic_index_in_dim(shaped[:, :, member], offset, axis=1, keepdims=False)
            )
        chosen = jnp.stack(chosen, axis=1)
        queries = chosen[:, :, 0]
        pairs = chosen[:, :, 1:]
        if segment > rows_here:
            levels = (segment // rows_here).bit_length() - 1
            flat_rows = collect_segment(pairs.reshape(count, -1), levels, seq_index)
            pairs = flat_rows.reshape(per_segment, heads_here, 2, head_dim)
            groups = 1
        else:
            groups = rows_here // segment
        grouped_queries = queries.reshape(groups, count // groups, heads_here, head_dim)
        grouped_pairs = pairs.reshape(groups, per_segment, heads_here, 2, head_dim)
        for member in range(heads_here):
            head_out, log_total = lax.map(
                lambda block_in: attend(block_in[0], block_in[1][:, 0], block_in[1][:, 1]),
                (grouped_queries[:, :, member], grouped_pairs[:, :, member]),
            )
            full_out, full_total = expand_rows(
                head_out.reshape(count, head_dim),
                log_total.reshape(count),
                offsets[member],
                dilation,
            )
            outputs[member].append(full_out)
            totals[member].append(full_total)
    merged = [
        merge_scales(outputs[member], totals[member]).astype(jnp.bfloat16)
        for member in range(heads_here)
    ]
    attention = jnp.stack(merged, axis=1).reshape(rows_here, heads_here * head_dim)
    regrouped = lax.all_to_all(attention, "head", split_axis=0, concat_axis=1, tiled=True)
    branch = jnp.dot(
        regrouped,
        lax.all_gather(out_weight, "head", axis=0, tiled=True),
        preferred_element_type=jnp.float32,
    )
    return (embedded + branch).astype(jnp.bfloat16)


HALF = 64


def iota(shape, dim):
    return lax.broadcasted_iota(jnp.int32, shape, dim)


def matmul(left, right, dims=((1,), (0,))):
    return lax.dot_general(left, right, (dims, ((), ())), preferred_element_type=jnp.float32)


def landed_place(slot, in_rows):
    middle, last = DILATIONS[1], DILATIONS[2]
    inner = last // middle
    run = in_rows // last
    return slot % middle * (inner * run) + slot // middle % inner * run + slot // last


def pack_kernel(seq_count, rows_ref, weight_ref, route_ref, *refs):
    blocks = refs[:seq_count]
    slots = refs[seq_count : 2 * seq_count]
    pick_ref = refs[-1]
    in_rows = rows_ref.shape[0]
    capacity = blocks[0].shape[0]

    @pl.when(pl.program_id(0) == 0)
    def _():
        me = lax.axis_index("seq")
        dest = route_ref[0:1, :]
        slot = route_ref[1:2, :]
        shift = jnp.where(dest < me, dest - me + seq_count, dest - me)
        hits = (iota((8, in_rows), 0) == shift).astype(jnp.float32)
        before = (iota((in_rows, in_rows), 0) < iota((in_rows, in_rows), 1)).astype(jnp.bfloat16)
        earlier = matmul(hits.astype(jnp.bfloat16), before)
        base = (iota((8, in_rows), 0) * capacity).astype(jnp.float32)
        place = jnp.sum(hits * (earlier + base), axis=0, keepdims=True).astype(jnp.int32)
        pick = iota((seq_count * capacity, in_rows), 0) == place
        pick_ref[...] = pick.astype(jnp.bfloat16)
        mark = (landed_place(slot, in_rows) + 1).astype(jnp.float32)
        marks = jnp.broadcast_to(mark, (8, in_rows)).astype(jnp.bfloat16)
        found = matmul(marks, pick_ref[...], ((1,), (1,))).astype(jnp.int32)
        for number in range(seq_count):
            slots[number][...] = found[0:1, number * capacity : (number + 1) * capacity]

    projected = matmul(rows_ref[...], weight_ref[...]).astype(jnp.bfloat16)
    packed = matmul(pick_ref[...], projected).astype(jnp.bfloat16)
    for number in range(seq_count):
        blocks[number][...] = packed[number * capacity : (number + 1) * capacity]


def pack(tile_rows, embed_weight, tile_route, seq_count):
    in_rows, depth = tile_rows.shape
    width = embed_weight.shape[1]
    capacity = 2 * in_rows // seq_count
    chunk = 256
    results = pl.pallas_call(
        functools.partial(pack_kernel, seq_count),
        grid=(width // chunk,),
        in_specs=[
            pl.BlockSpec((in_rows, depth), lambda step: (0, 0)),
            pl.BlockSpec((depth, chunk), lambda step: (0, step)),
            pl.BlockSpec((2, in_rows), lambda step: (0, 0)),
        ],
        out_specs=[pl.BlockSpec((capacity, chunk), lambda step: (0, step))] * seq_count
        + [pl.BlockSpec((1, capacity), lambda step: (0, 0))] * seq_count,
        out_shape=[jax.ShapeDtypeStruct((capacity, width), jnp.bfloat16)] * seq_count
        + [jax.ShapeDtypeStruct((1, capacity), jnp.int32)] * seq_count,
        scratch_shapes=[pltpu.VMEM((seq_count * capacity, in_rows), jnp.bfloat16)],
        cost_estimate=cost(2 * in_rows * width * (depth + seq_count * capacity)),
        name="pack",
    )(tile_rows, embed_weight, tile_route.T)
    return results[:seq_count], results[seq_count:]


def cost(flops):
    return pl.CostEstimate(flops=flops, bytes_accessed=1 << 20, transcendentals=0)


def land_kernel(count, *refs):
    blocks, slots = refs[:count], refs[count : 2 * count]
    gain_ref, rows_ref, normed_ref = refs[2 * count :]
    in_rows = rows_ref.shape[0]
    capacity = blocks[0].shape[0]
    rows = jnp.zeros(rows_ref.shape, jnp.float32)
    for block, slot in zip(blocks, slots):
        here = (iota((in_rows, capacity), 0) + 1 == slot[...]).astype(jnp.bfloat16)
        rows = rows + matmul(here, block[...])
    rows_ref[...] = rows.astype(jnp.bfloat16)
    normed_ref[...] = layer_norm(rows, gain_ref[...])


def land(blocks, slots, norm_gain, in_rows):
    count = len(blocks)
    capacity, width = blocks[0].shape
    shape = jax.ShapeDtypeStruct((in_rows, width), jnp.bfloat16)
    return pl.pallas_call(
        functools.partial(land_kernel, count),
        out_shape=[shape, shape],
        cost_estimate=cost(2 * in_rows * width * count * capacity),
        name="land",
    )(*blocks, *slots, norm_gain.reshape(1, width))


def turn_kernel(rows_ref, *refs):
    pieces = refs[:-2]
    turned_ref, weight_ref = refs[-2:]
    turned_ref[...] = rows_ref[...].T
    depth = pieces[0].shape[0]
    for number, piece in enumerate(pieces):
        weight_ref[:, number * depth : (number + 1) * depth] = piece[...].T


def turn(rows, pieces):
    width = rows.shape[1]
    inner = sum(piece.shape[0] for piece in pieces)
    return pl.pallas_call(
        turn_kernel,
        out_shape=[
            jax.ShapeDtypeStruct((width, rows.shape[0]), jnp.bfloat16),
            jax.ShapeDtypeStruct((width, inner), jnp.bfloat16),
        ],
        cost_estimate=cost(2 * rows.shape[0] * width * 512),
        name="turn",
    )(rows, *pieces)


def project_block(rows, weight, head_dim):
    out = matmul(rows, weight)
    third = out.shape[1] // 3
    lanes = iota((1, out.shape[1]), 1)
    ones = (lanes >= 2 * third) & (lanes % HALF == head_dim)
    return (out + ones.astype(jnp.float32)).astype(jnp.bfloat16)


def first_qkv_kernel(head_dim, one_ref, two_ref, weight_ref, out_ref):
    in_rows = one_ref.shape[0]
    weight = weight_ref[...]
    out_ref[:in_rows] = project_block(one_ref[...], weight, head_dim)
    out_ref[in_rows:] = project_block(two_ref[...], weight, head_dim)


def second_qkv_kernel(head_dim, heads_here, one_ref, two_ref, weight_ref, first_ref, out_ref, far_ref):
    in_rows = one_ref.shape[0]
    first_qkv_kernel(head_dim, one_ref, two_ref, weight_ref, out_ref)
    middle, last = DILATIONS[1], DILATIONS[2]
    run = in_rows // last
    third = heads_here * HALF
    inner = lax.axis_index("head") % (last // middle)
    low = iota((1, 2 * HALF), 1) < HALF
    for number in range(4):
        source = first_ref if number < 2 else out_ref
        start = number % 2 * in_rows
        for part in range(2):
            for pair in range(heads_here // 2):
                column = (1 + part) * third + pair * 2 * HALF
                both = []
                for member in (2 * pair, 2 * pair + 1):
                    row = start + member * (in_rows // middle) + inner * run
                    both.append(
                        source[pl.ds(pl.multiple_of(row, run), run), column : column + 2 * HALF]
                    )
                far_ref[
                    number * run : (number + 1) * run,
                    part * third + pair * 2 * HALF : part * third + (pair + 1) * 2 * HALF,
                ] = jnp.where(low, both[0], both[1])


def first_qkv(one, two, weight, head_dim):
    in_rows, width = one.shape
    return pl.pallas_call(
        functools.partial(first_qkv_kernel, head_dim),
        out_shape=jax.ShapeDtypeStruct((2 * in_rows, weight.shape[1]), jnp.bfloat16),
        cost_estimate=cost(4 * in_rows * width * weight.shape[1]),
        name="first_qkv",
    )(one, two, weight)


def second_qkv(one, two, weight, first, head_dim, heads_here):
    in_rows, width = one.shape
    return pl.pallas_call(
        functools.partial(second_qkv_kernel, head_dim, heads_here),
        out_shape=[
            jax.ShapeDtypeStruct((2 * in_rows, weight.shape[1]), jnp.bfloat16),
            jax.ShapeDtypeStruct((4 * in_rows // DILATIONS[2], 2 * heads_here * HALF), jnp.bfloat16),
        ],
        cost_estimate=cost(4 * in_rows * width * weight.shape[1]),
        name="second_qkv",
    )(one, two, weight, first)


def softmax_product(scores, scale, turned):
    top = functools.reduce(jnp.maximum, [jnp.max(each, axis=0, keepdims=True) for each in scores])
    total = None
    for each, values in zip(scores, turned):
        weights = jnp.exp2(each * scale - top * scale).astype(jnp.bfloat16)
        product = matmul(values, weights)
        total = product if total is None else total + product
    return total, top


def attention_kernel(head_dim, heads_here, first_ref, second_ref, *refs):
    fars, outs = refs[:-4], refs[-4:]
    in_rows = first_ref.shape[0] // 2
    middle, last = DILATIONS[1], DILATIONS[2]
    wide = in_rows // middle
    run = in_rows // last
    third = heads_here * HALF
    scale = 1.4426950408889634 * head_dim ** (-0.5)
    inner = lax.axis_index("head") % (last // middle)
    lanes = iota((1, 2 * HALF), 1)
    chosen = iota((1, in_rows), 1) // run % (last // middle) == inner
    sources = [(first_ref, 0), (first_ref, in_rows), (second_ref, 0), (second_ref, in_rows)]
    for pair in range(heads_here // 2):
        span = slice(pair * 2 * HALF, (pair + 1) * 2 * HALF)
        keys_at = slice(third + span.start, third + span.stop)
        values_at = slice(2 * third + span.start, 2 * third + span.stop)
        block_keys = [source[start : start + in_rows, keys_at] for source, start in sources]
        block_turned = [source[start : start + in_rows, values_at].T for source, start in sources]
        far_keys = jnp.concatenate([far[:, span] for far in fars], axis=0)
        far_turned = jnp.concatenate(
            [far[:, third + span.start : third + span.stop] for far in fars], axis=0
        ).T
        for side in range(2):
            member = 2 * pair + side
            mine = (lanes // HALF == side).astype(jnp.bfloat16)
            held = slice(side * HALF, (side + 1) * HALF)
            picked = [
                slice(start + member * wide, start + (member + 1) * wide) for _, start in sources
            ]

            def gathered(columns):
                return jnp.concatenate(
                    [source[rows, columns] for (source, _), rows in zip(sources, picked)], axis=0
                )

            picked_queries = gathered(span) * mine
            near = matmul(gathered(keys_at), picked_queries, ((1,), (1,)))
            far = matmul(far_keys, picked_queries, ((1,), (1,)))
            far = jnp.where(chosen, far, -1e30)
            wide_total, wide_top = softmax_product(
                [near, far], scale, [gathered(values_at).T[held], far_turned[held]]
            )
            for number in range(4):
                source, start = sources[number]
                queries = source[start : start + in_rows, span] * mine
                scores = matmul(block_keys[number], queries, ((1,), (1,)))
                total, top = softmax_product([scores], scale, [block_turned[number][held]])
                extra, extra_top = place_lanes(wide_total, wide_top, number, member, wide)
                tile = member * wide // 128 * 128
                at = slice(tile, tile + 128)
                inside = iota((1, 128), 1) // wide == member % (128 // wide)
                extra_top = jnp.where(inside, extra_top, -1e30)
                peak = jnp.maximum(top[:, at], extra_top)
                old = jnp.exp2((top[:, at] - peak) * scale)
                new = jnp.exp2((extra_top - peak) * scale)
                merged = total[:, at] * old + jnp.where(inside, extra * new, 0.0)
                parts = []
                for other in range(0, in_rows, 128):
                    parts.append(merged if other == tile else total[:, other : other + 128])
                rows = slice(member * head_dim, (member + 1) * head_dim)
                for index, part in enumerate(parts):
                    done = part[:head_dim] / part[head_dim : head_dim + 1]
                    outs[number][rows, index * 128 : (index + 1) * 128] = done.astype(jnp.bfloat16)


def place_lanes(total, top, number, member, wide):
    tile = number * wide // 128 * 128
    shift = (member * wide - number * wide) % 128
    total, top = total[:, tile : tile + 128], top[:, tile : tile + 128]
    if shift:
        total = pltpu.roll(total, shift, 1)
        top = pltpu.roll(jnp.broadcast_to(top, (8, 128)), shift, 1)[:1]
    return total, top


def attention_blocks(first, second, fars, head_dim, heads_here):
    in_rows = first.shape[0] // 2
    out = jax.ShapeDtypeStruct((heads_here * head_dim, in_rows), jnp.bfloat16)
    return pl.pallas_call(
        functools.partial(attention_kernel, head_dim, heads_here),
        out_shape=[out] * 4,
        cost_estimate=cost(24 * 4 * in_rows * in_rows * 128),
        name="attention",
    )(first, second, *fars)


def finish_kernel(turned_ref, weight_ref, *refs):
    pieces, out_ref = refs[:-1], refs[-1]
    joined = jnp.concatenate([piece[...] for piece in pieces], axis=0)
    branch = matmul(weight_ref[...], joined)
    mixed = (turned_ref[...].astype(jnp.float32) + branch).astype(jnp.bfloat16)
    in_rows = out_ref.shape[0]
    square = (in_rows, in_rows)
    back = landed_place(iota(square, 0), in_rows) == iota(square, 1)
    out_ref[...] = matmul(back.astype(jnp.bfloat16), mixed, ((1,), (1,))).astype(jnp.bfloat16)


def finish(turned, weight, pieces):
    width, in_rows = turned.shape
    return pl.pallas_call(
        finish_kernel,
        out_shape=jax.ShapeDtypeStruct((in_rows, width), jnp.bfloat16),
        cost_estimate=cost(2 * in_rows * width * (width + in_rows)),
        name="finish",
    )(turned, weight, *pieces)


def across(block, bit):
    count = lax.axis_size("head")
    return lax.ppermute(block, "head", [(member, member ^ bit) for member in range(count)])


def shifted(block, shift):
    count = lax.axis_size("seq")
    return lax.ppermute(block, "seq", [(member, (member + shift) % count) for member in range(count)])


def all_four(block):
    beside = across(block, 1)
    over = across(block, 2)
    return [block, beside, over, across(over, 1)]


def fits(tile_rows, qkv_weight):
    in_rows = tile_rows.shape[0]
    seq_count, head_count = lax.axis_size("seq"), lax.axis_size("head")
    heads_here, head_dim = qkv_weight.shape[1], qkv_weight.shape[3]
    rows_here = in_rows * head_count
    total_rows = rows_here * seq_count
    segments = [total_rows // fraction for fraction in FRACTIONS]
    return (
        segments == [in_rows, rows_here, total_rows]
        and head_count == 4
        and seq_count <= 8
        and heads_here == DILATIONS[1] == DILATIONS[2] // DILATIONS[1]
        and in_rows == 4 * HALF
        and head_dim % 16 == 0
        and head_dim < HALF
    )


def fast(tile_rows, tile_route, embed_weight, norm_gain, qkv_weight, out_weight):
    seq_count = lax.axis_size("seq")
    in_rows = tile_rows.shape[0]
    width = embed_weight.shape[1]
    heads_here, head_dim = qkv_weight.shape[1], qkv_weight.shape[3]
    blocks, slots = pack(tile_rows, embed_weight, tile_route, seq_count)
    order = sorted(range(1, seq_count), key=lambda shift: -min(shift, seq_count - shift))
    moved_slots = [shifted(slots[shift], shift) for shift in order]
    moved = [shifted(blocks[shift], shift) for shift in order]
    pieces = all_four(out_weight)
    by_kind = jnp.transpose(qkv_weight, (0, 2, 1, 3))
    weight = jnp.pad(by_kind, ((0, 0), (0, 0), (0, 0), (0, HALF - head_dim))).reshape(width, -1)
    rows, normed = land([blocks[0]] + moved, [slots[0]] + moved_slots, norm_gain, in_rows)
    one, two, three, four = all_four(normed)
    turned, turned_weight = turn(rows, pieces)
    first = first_qkv(one, two, weight, head_dim)
    second, far = second_qkv(three, four, weight, first, head_dim, heads_here)
    fars = [far] + [shifted(far, shift) for shift in order]
    parts = attention_blocks(first, second, fars, head_dim, heads_here)
    joined = [parts[0]] + [across(parts[bit], bit) for bit in range(1, 4)]
    return finish(turned, turned_weight, joined)


def local(tile_rows, tile_route, embed_weight, norm_gain, qkv_weight, out_weight):
    run = fast if fits(tile_rows, qkv_weight) else general
    return run(tile_rows, tile_route, embed_weight, norm_gain, qkv_weight, out_weight)


def solution(mesh):
    return jax.shard_map(
        local,
        mesh=mesh,
        in_specs=(
            P(("groups", "seq", "head"), None),
            P(("groups", "seq", "head"), None),
            P(),
            P(),
            P(None, "head", None, None),
            P("head", None),
        ),
        out_specs=P(("groups", "seq", "head"), None),
        check_vma=False,
    )
```

```python
import functools

import jax
import jax.numpy as jnp
from jax import lax
from jax.experimental import pallas as pl
from jax.experimental.pallas import tpu as pltpu

from jax.sharding import PartitionSpec as P


EPSILON = 1e-05
DILATIONS = (1, 4, 16)
FRACTIONS = (16, 4, 1)


def from_partner(block, axis, apart):
    count = lax.axis_size(axis)
    route = []
    for low in range(count):
        high = low | 1 << apart
        if high != low and high < count:
            route += [(low, high), (high, low)]
    return lax.ppermute(block, axis, route)


def layer_norm(rows, gain):
    row_mean = jnp.mean(rows, axis=-1, keepdims=True)
    centered = rows - row_mean
    row_var = jnp.mean(centered * centered, axis=-1, keepdims=True)
    return (centered * lax.rsqrt(row_var + EPSILON) * gain).astype(jnp.bfloat16)


def attend_block(queries, key_rows, values):
    score_scale = queries.shape[-1] ** (-0.5)
    scores = jnp.dot(queries, key_rows.T, preferred_element_type=jnp.float32) * score_scale
    row_max = jnp.max(scores, axis=-1)
    expo = jnp.exp(scores - row_max[:, None])
    denominator = jnp.sum(expo, axis=-1)
    weights = (expo / denominator[:, None]).astype(jnp.bfloat16)
    head_out = jnp.dot(weights, values, preferred_element_type=jnp.float32)
    return (head_out, row_max + jnp.log(denominator))


def attend(queries, key_rows, values):
    count = queries.shape[0]
    if count > 512 and count % 512 == 0:
        blocks = queries.reshape(count // 512, 512, queries.shape[1])
        head_out, log_total = lax.map(
            lambda block_in: attend_block(block_in, key_rows, values), blocks
        )
        return (head_out.reshape(count, -1), log_total.reshape(count))
    return attend_block(queries, key_rows, values)


def expand_rows(head_out, log_total, offset, dilation):
    count = head_out.shape[0]
    pick_mask = jnp.arange(dilation, dtype=jnp.int32) == offset
    full_out = jnp.where(pick_mask[None, :, None], head_out[:, None, :], 0.0).reshape(
        count * dilation, -1
    )
    full_total = jnp.where(pick_mask[None, :], log_total[:, None], -1e30).reshape(count * dilation)
    return (full_out, full_total)


def merge_scales(outputs, totals):
    row_max = jnp.maximum(jnp.maximum(totals[0], totals[1]), totals[2])
    numer = jnp.zeros_like(outputs[0])
    denom = jnp.zeros_like(totals[0])
    for full_out, full_total in zip(outputs, totals):
        factor = jnp.exp(full_total - row_max)
        numer = numer + factor[:, None] * full_out
        denom = denom + factor
    return numer / denom[:, None]


def collect_segment(flat_rows, levels, seq_index):
    for level in range(levels):
        partner = from_partner(flat_rows, "seq", level)
        upper_half = seq_index >> level & 1 == 1
        lower_rows = jnp.where(upper_half, partner, flat_rows)
        upper_rows = jnp.where(upper_half, flat_rows, partner)
        flat_rows = jnp.concatenate([lower_rows, upper_rows], axis=0)
    return flat_rows


def general(tile_rows, tile_route, embed_weight, norm_gain, qkv_weight, out_weight):
    seq_count = lax.axis_size("seq")
    seq_index = lax.axis_index("seq")
    in_rows = tile_rows.shape[0]
    width = embed_weight.shape[1]
    capacity = 2 * in_rows // seq_count
    projected = jnp.dot(tile_rows, embed_weight, preferred_element_type=jnp.float32).astype(
        jnp.bfloat16
    )
    dest_seq = tile_route[:, 0]
    slot_index = tile_route[:, 1]
    owner_hits = (dest_seq[:, None] == jnp.arange(seq_count, dtype=jnp.int32)[None, :]).astype(
        jnp.int32
    )
    earlier = jnp.cumsum(owner_hits, axis=0) - owner_hits
    owner_rank = jnp.sum(earlier * owner_hits, axis=1)
    buffer_place = dest_seq * capacity + owner_rank
    send_pick = jnp.arange(seq_count * capacity, dtype=jnp.int32)[:, None] == buffer_place[None, :]
    outgoing = jnp.dot(
        send_pick.astype(jnp.bfloat16), projected, preferred_element_type=jnp.float32
    ).astype(jnp.bfloat16)
    outgoing_slot = jnp.sum(jnp.where(send_pick, slot_index[None, :] + 1, 0), axis=1)
    arrived, arrived_slot = (
        lax.all_to_all(
            outgoing.reshape(seq_count, capacity, width),
            "seq",
            split_axis=0,
            concat_axis=0,
            tiled=True,
        ),
        lax.all_to_all(
            outgoing_slot.reshape(seq_count, capacity),
            "seq",
            split_axis=0,
            concat_axis=0,
            tiled=True,
        ),
    )
    landing = jnp.arange(in_rows, dtype=jnp.int32)[:, None] + 1 == arrived_slot.reshape(-1)[None, :]
    embedded = jnp.dot(
        landing.astype(jnp.bfloat16), arrived.reshape(-1, width), preferred_element_type=jnp.float32
    )
    normed = layer_norm(embedded, norm_gain)
    heads_here = qkv_weight.shape[1]
    head_dim = qkv_weight.shape[3]
    weight_flat = qkv_weight.reshape(width, -1)
    qkv = jnp.dot(
        lax.all_gather(normed, "head", axis=0, tiled=True),
        weight_flat,
        preferred_element_type=jnp.float32,
    ).astype(jnp.bfloat16)
    rows_here = qkv.shape[0]
    qkv = qkv.reshape(rows_here, heads_here, 3, head_dim)
    first_head = lax.axis_index("head") * heads_here
    total_rows = rows_here * seq_count
    outputs = [[] for _ in range(heads_here)]
    totals = [[] for _ in range(heads_here)]
    for fraction, dilation in zip(FRACTIONS, DILATIONS):
        segment = total_rows // fraction
        per_segment = segment // dilation
        count = rows_here // dilation
        shaped = qkv.reshape(count, dilation, heads_here, 3, head_dim)
        offsets = []
        chosen = []
        for member in range(heads_here):
            offset = (first_head + member) % dilation
            offsets.append(offset)
            chosen.append(
                lax.dynamic_index_in_dim(shaped[:, :, member], offset, axis=1, keepdims=False)
            )
        chosen = jnp.stack(chosen, axis=1)
        queries = chosen[:, :, 0]
        pairs = chosen[:, :, 1:]
        if segment > rows_here:
            levels = (segment // rows_here).bit_length() - 1
            flat_rows = collect_segment(pairs.reshape(count, -1), levels, seq_index)
            pairs = flat_rows.reshape(per_segment, heads_here, 2, head_dim)
            groups = 1
        else:
            groups = rows_here // segment
        grouped_queries = queries.reshape(groups, count // groups, heads_here, head_dim)
        grouped_pairs = pairs.reshape(groups, per_segment, heads_here, 2, head_dim)
        for member in range(heads_here):
            head_out, log_total = lax.map(
                lambda block_in: attend(block_in[0], block_in[1][:, 0], block_in[1][:, 1]),
                (grouped_queries[:, :, member], grouped_pairs[:, :, member]),
            )
            full_out, full_total = expand_rows(
                head_out.reshape(count, head_dim),
                log_total.reshape(count),
                offsets[member],
                dilation,
            )
            outputs[member].append(full_out)
            totals[member].append(full_total)
    merged = [
        merge_scales(outputs[member], totals[member]).astype(jnp.bfloat16)
        for member in range(heads_here)
    ]
    attention = jnp.stack(merged, axis=1).reshape(rows_here, heads_here * head_dim)
    regrouped = lax.all_to_all(attention, "head", split_axis=0, concat_axis=1, tiled=True)
    branch = jnp.dot(
        regrouped,
        lax.all_gather(out_weight, "head", axis=0, tiled=True),
        preferred_element_type=jnp.float32,
    )
    return (embedded + branch).astype(jnp.bfloat16)


HALF = 64


def iota(shape, dim):
    return lax.broadcasted_iota(jnp.int32, shape, dim)


def matmul(left, right, dims=((1,), (0,))):
    return lax.dot_general(left, right, (dims, ((), ())), preferred_element_type=jnp.float32)


def landed_place(slot, in_rows):
    middle, last = DILATIONS[1], DILATIONS[2]
    inner = last // middle
    run = in_rows // last
    return slot % middle * (inner * run) + slot // middle % inner * run + slot // last


def pack_kernel(seq_count, rows_hbm, weight_hbm, route_ref, *refs):
    blocks = refs[:seq_count]
    picks = refs[seq_count:-3]
    rows_ref, weight_ref, arrived = refs[-3:]
    in_rows = rows_ref.shape[0]
    chunks, _, chunk = weight_ref.shape
    capacity = 2 * in_rows // seq_count
    first = weight_hbm.shape[1] - chunks * chunk if not picks else 0
    rows_copy = pltpu.make_async_copy(rows_hbm, rows_ref, arrived.at[chunks])
    rows_copy.start()
    copies = []
    for number in range(chunks):
        columns = slice(first + number * chunk, first + (number + 1) * chunk)
        copies.append(
            pltpu.make_async_copy(
                weight_hbm.at[:, columns], weight_ref.at[number], arrived.at[number]
            )
        )
        copies[number].start()

    if picks:
        me = lax.axis_index("seq")
        dest = route_ref[0:1, :]
        slot = route_ref[1:2, :]
        shift = jnp.where(dest < me, dest - me + seq_count, dest - me)
        hits = (iota((8, in_rows), 0) == shift).astype(jnp.float32)
        before = (iota((in_rows, in_rows), 0) < iota((in_rows, in_rows), 1)).astype(jnp.bfloat16)
        earlier = matmul(hits.astype(jnp.bfloat16), before)
        base = (iota((8, in_rows), 0) * capacity).astype(jnp.float32)
        place = jnp.sum(hits * (earlier + base), axis=0, keepdims=True).astype(jnp.int32)
        pick = (iota((seq_count * capacity, in_rows), 0) == place).astype(jnp.bfloat16)
        picks[0][...] = pick
        mark = (landed_place(slot, in_rows) + 1).astype(jnp.float32)
        marks = jnp.broadcast_to(mark, (8, in_rows)).astype(jnp.bfloat16)
        found = matmul(marks, pick, ((1,), (1,))).astype(jnp.bfloat16)
        for number in range(seq_count):
            spare = (blocks[number].shape[0] - capacity, blocks[number].shape[1])
            blocks[number][capacity:] = jnp.zeros(spare, jnp.bfloat16)
            blocks[number][capacity : capacity + 8, :capacity] = found[
                :, number * capacity : (number + 1) * capacity
            ]
    else:
        pick = route_ref[...]

    rows_copy.wait()
    for step in range(chunks):
        copies[step].wait()
        projected = matmul(rows_ref[...], weight_ref[step]).astype(jnp.bfloat16)
        packed = matmul(pick, projected).astype(jnp.bfloat16)
        columns = slice(step * chunk, (step + 1) * chunk)
        for number in range(seq_count):
            blocks[number][:capacity, columns] = packed[number * capacity : (number + 1) * capacity]


def pack(tile_rows, embed_weight, route, columns, seq_count):
    in_rows, depth = tile_rows.shape
    capacity = 2 * in_rows // seq_count
    chunk = 256
    lead = route.dtype == jnp.int32
    hbm = pl.BlockSpec(memory_space=pltpu.HBM)
    rows = capacity + 8 if lead else capacity
    shapes = [jax.ShapeDtypeStruct((rows, columns), jnp.bfloat16)] * seq_count
    if lead:
        shapes.append(jax.ShapeDtypeStruct((seq_count * capacity, in_rows), jnp.bfloat16))
    results = pl.pallas_call(
        functools.partial(pack_kernel, seq_count),
        in_specs=[hbm, hbm, pl.BlockSpec(memory_space=pltpu.VMEM)],
        out_shape=shapes,
        scratch_shapes=[
            pltpu.VMEM((in_rows, depth), jnp.bfloat16),
            pltpu.VMEM((columns // chunk, depth, chunk), jnp.bfloat16),
            pltpu.SemaphoreType.DMA((columns // chunk + 1,)),
        ],
        cost_estimate=cost(2 * in_rows * columns * (depth + seq_count * capacity)),
        compiler_params=pltpu.CompilerParams(vmem_limit_bytes=62 << 20),
    )(tile_rows, embed_weight, route)
    return results[:seq_count], results[-1]


LIMIT = pltpu.CompilerParams(vmem_limit_bytes=16 << 20)


def cost(flops):
    return pl.CostEstimate(flops=flops, bytes_accessed=1 << 20, transcendentals=0)


def land_kernel(count, *refs):
    blocks = refs[:count]
    rows_ref, here_ref = refs[count:]
    in_rows = rows_ref.shape[0]
    capacity = 2 * in_rows // count
    rows = jnp.zeros(rows_ref.shape, jnp.float32)
    for number, block in enumerate(blocks):
        slot = block[capacity : capacity + 8, :capacity].astype(jnp.float32)[:1]
        here = ((iota((in_rows, capacity), 0) + 1).astype(jnp.float32) == slot).astype(jnp.bfloat16)
        here_ref[:, number * capacity : (number + 1) * capacity] = here
        rows = rows + matmul(here, block[:capacity])
    rows_ref[...] = rows.astype(jnp.bfloat16)


def land(blocks, in_rows):
    count = len(blocks)
    capacity = 2 * in_rows // count
    width = blocks[0].shape[1]
    return pl.pallas_call(
        functools.partial(land_kernel, count),
        out_shape=[
            jax.ShapeDtypeStruct((in_rows, width), jnp.bfloat16),
            jax.ShapeDtypeStruct((in_rows, count * capacity), jnp.bfloat16),
        ],
        cost_estimate=cost(2 * in_rows * width * count * capacity),
        compiler_params=LIMIT,
        name="land_lead",
    )(*blocks)


def land_more_kernel(here_ref, *refs):
    blocks, rows_ref = refs[:-1], refs[-1]
    capacity = blocks[0].shape[0]
    rows = jnp.zeros(rows_ref.shape, jnp.float32)
    for number, block in enumerate(blocks):
        here = here_ref[:, number * capacity : (number + 1) * capacity]
        rows = rows + matmul(here, block[...])
    rows_ref[...] = rows.astype(jnp.bfloat16)


def land_more(here, blocks):
    in_rows, total = here.shape
    width = blocks[0].shape[1]
    return pl.pallas_call(
        land_more_kernel,
        out_shape=jax.ShapeDtypeStruct((in_rows, width), jnp.bfloat16),
        cost_estimate=cost(2 * in_rows * width * total),
        compiler_params=LIMIT,
        name="land_rest",
    )(here, *blocks)


def turn_kernel(down, *refs):
    pieces, out_ref = refs[:-1], refs[-1]
    start = 0
    for piece in pieces:
        depth = piece.shape[1 if down else 0]
        if down:
            out_ref[start : start + depth] = piece[...].T
        else:
            out_ref[:, start : start + depth] = piece[...].T
        start += depth


def turn(pieces, down):
    rows = sum(piece.shape[0] for piece in pieces)
    columns = sum(piece.shape[1] for piece in pieces)
    shape = (columns, pieces[0].shape[0]) if down else (pieces[0].shape[1], rows)
    return pl.pallas_call(
        functools.partial(turn_kernel, down),
        out_shape=jax.ShapeDtypeStruct(shape, jnp.bfloat16),
        cost_estimate=cost(len(pieces) * 100_000_000),
        compiler_params=LIMIT,
    )(*pieces)


def project_block(rows, weight, head_dim):
    out = matmul(rows, weight)
    third = out.shape[1] // 3
    lanes = iota((1, out.shape[1]), 1)
    ones = (lanes >= 2 * third) & (lanes % HALF == head_dim)
    return (out + ones.astype(jnp.float32)).astype(jnp.bfloat16)


def qkv_kernel(head_dim, heads_here, lead_ref, rest_ref, gain_ref, weight_ref, out_ref, far_ref):
    in_rows = lead_ref.shape[0]
    rows = jnp.concatenate([lead_ref[...], rest_ref[...]], axis=1).astype(jnp.float32)
    normed = layer_norm(rows, gain_ref[...])
    out_ref[...] = project_block(normed, weight_ref[...], head_dim)
    middle, last = DILATIONS[1], DILATIONS[2]
    run = in_rows // last
    third = heads_here * HALF
    inner = lax.axis_index("head") % (last // middle)
    low = iota((1, 2 * HALF), 1) < HALF
    for column in range(third, 3 * third, 2 * HALF):
        both = []
        for side in range(2):
            member = column % third // HALF + side
            row = member * (in_rows // middle) + inner * run
            both.append(out_ref[pl.ds(pl.multiple_of(row, run), run), column : column + 2 * HALF])
        far_ref[:, column - third : column - third + 2 * HALF] = jnp.where(low, both[0], both[1])


def near_kernel(head_dim, heads_here, qkv_ref, out_ref):
    in_rows = qkv_ref.shape[0]
    third = heads_here * HALF
    scale = LOG2E * head_dim ** (-0.5)
    lanes = iota((1, 2 * HALF), 1)
    for first in range(0, third, 2 * HALF):
        keys = qkv_ref[:, third + first : third + first + 2 * HALF]
        turned = qkv_ref[:, 2 * third + first : 2 * third + first + 2 * HALF].T
        for side in range(2):
            mine = (lanes // HALF == side).astype(jnp.bfloat16)
            queries = qkv_ref[:, first : first + 2 * HALF] * mine
            scores = matmul(keys, queries, ((1,), (1,)))
            values = turned[side * HALF : (side + 1) * HALF]
            total, top = softmax_product([scores], scale, [values])
            start = first + side * HALF
            out_ref[start : start + HALF] = total
            out_ref[start + HALF - 8 : start + HALF] = jnp.broadcast_to(top, (8, in_rows))


def qkv_of(halves, gain, weight, head_dim, heads_here):
    in_rows = halves[0].shape[0]
    return pl.pallas_call(
        functools.partial(qkv_kernel, head_dim, heads_here),
        out_shape=[
            jax.ShapeDtypeStruct((in_rows, weight.shape[1]), jnp.bfloat16),
            jax.ShapeDtypeStruct((in_rows // DILATIONS[2], 2 * heads_here * HALF), jnp.bfloat16),
        ],
        cost_estimate=cost(2 * in_rows * weight.shape[0] * weight.shape[1]),
        compiler_params=LIMIT,
    )(*halves, gain, weight)


def near(qkv, head_dim, heads_here):
    in_rows = qkv.shape[0]
    return pl.pallas_call(
        functools.partial(near_kernel, head_dim, heads_here),
        out_shape=jax.ShapeDtypeStruct((heads_here * HALF, in_rows), jnp.float32),
        cost_estimate=cost(heads_here * 8 * in_rows * in_rows * 128),
        compiler_params=LIMIT,
    )(qkv)


def softmax_product(scores, scale, turned):
    top = functools.reduce(jnp.maximum, [jnp.max(each, axis=0, keepdims=True) for each in scores])
    total = None
    for each, values in zip(scores, turned):
        weights = jnp.exp2(each * scale - top * scale).astype(jnp.bfloat16)
        product = matmul(values, weights)
        total = product if total is None else total + product
    return total, top


LOG2E = 1.4426950408889634


def wide_kernel(head_dim, heads_here, *refs):
    sources, fars, nears, outs = refs[:4], refs[4:-8], refs[-8:-4], refs[-4:]
    in_rows = sources[0].shape[0]
    middle, last = DILATIONS[1], DILATIONS[2]
    wide = in_rows // middle
    run = in_rows // last
    third = heads_here * HALF
    scale = LOG2E * head_dim ** (-0.5)
    inner = lax.axis_index("head") % (last // middle)
    lanes = iota((1, 2 * HALF), 1)
    chosen = iota((1, in_rows), 1) // run % (last // middle) == inner
    for pair in range(heads_here // 2):
        span = slice(pair * 2 * HALF, (pair + 1) * 2 * HALF)
        keys_at = slice(third + span.start, third + span.stop)
        values_at = slice(2 * third + span.start, 2 * third + span.stop)
        far_keys = jnp.concatenate([far[:, span] for far in fars], axis=0)
        far_turned = jnp.concatenate(
            [far[:, third + span.start : third + span.stop] for far in fars], axis=0
        ).T
        for side in range(2):
            member = 2 * pair + side
            mine = (lanes // HALF == side).astype(jnp.bfloat16)
            held = slice(side * HALF, (side + 1) * HALF)
            picked = slice(member * wide, (member + 1) * wide)

            def gathered(columns):
                return jnp.concatenate([source[picked, columns] for source in sources], axis=0)

            picked_queries = gathered(span) * mine
            middle_scores = matmul(gathered(keys_at), picked_queries, ((1,), (1,)))
            far_scores = matmul(far_keys, picked_queries, ((1,), (1,)))
            far_scores = jnp.where(chosen, far_scores, -1e30)
            wide_total, wide_top = softmax_product(
                [middle_scores, far_scores], scale, [gathered(values_at).T[held], far_turned[held]]
            )
            for number in range(4):
                base = member * HALF
                total = nears[number][base : base + HALF]
                top = nears[number][base + HALF - 8 : base + HALF][:1]
                extra, extra_top = place_lanes(wide_total, wide_top, number, member, wide)
                tile = member * wide // 128 * 128
                at = slice(tile, tile + 128)
                inside = iota((1, 128), 1) // wide == member % (128 // wide)
                extra_top = jnp.where(inside, extra_top, -1e30)
                peak = jnp.maximum(top[:, at], extra_top)
                old = jnp.exp2((top[:, at] - peak) * scale)
                new = jnp.exp2((extra_top - peak) * scale)
                merged = total[:, at] * old + jnp.where(inside, extra * new, 0.0)
                rows = slice(member * head_dim, (member + 1) * head_dim)
                for other in range(0, in_rows, 128):
                    part = merged if other == tile else total[:, other : other + 128]
                    done = part[:head_dim] / part[head_dim : head_dim + 1]
                    outs[number][rows, other : other + 128] = done.astype(jnp.bfloat16)


def place_lanes(total, top, number, member, wide):
    tile = number * wide // 128 * 128
    shift = (member * wide - number * wide) % 128
    total, top = total[:, tile : tile + 128], top[:, tile : tile + 128]
    if shift:
        total = pltpu.roll(total, shift, 1)
        top = pltpu.roll(jnp.broadcast_to(top, (8, 128)), shift, 1)[:1]
    return total, top


def attention_blocks(sources, fars, nears, head_dim, heads_here):
    in_rows = sources[0].shape[0]
    out = jax.ShapeDtypeStruct((heads_here * head_dim, in_rows), jnp.bfloat16)
    return pl.pallas_call(
        functools.partial(wide_kernel, head_dim, heads_here),
        out_shape=[out] * 4,
        cost_estimate=cost(8 * 4 * in_rows * in_rows * 128),
        compiler_params=LIMIT,
        name="wide",
    )(*sources, *fars, *nears)


def finish_kernel(turned_ref, weight_ref, *refs):
    pieces, out_ref = refs[:-1], refs[-1]
    joined = jnp.concatenate([piece[...] for piece in pieces], axis=0)
    branch = matmul(weight_ref[...], joined)
    mixed = (turned_ref[...].astype(jnp.float32) + branch).astype(jnp.bfloat16)
    in_rows = out_ref.shape[0]
    square = (in_rows, in_rows)
    back = landed_place(iota(square, 0), in_rows) == iota(square, 1)
    out_ref[...] = matmul(back.astype(jnp.bfloat16), mixed, ((1,), (1,))).astype(jnp.bfloat16)


def finish(turned, weight, pieces):
    width, in_rows = turned.shape
    return pl.pallas_call(
        finish_kernel,
        out_shape=jax.ShapeDtypeStruct((in_rows, width), jnp.bfloat16),
        cost_estimate=cost(2 * in_rows * width * (width + in_rows)),
        compiler_params=LIMIT,
        name="finish",
    )(turned, weight, *pieces)


def across(block, bit):
    count = lax.axis_size("head")
    return lax.ppermute(block, "head", [(member, member ^ bit) for member in range(count)])


def shifted(block, shift):
    count = lax.axis_size("seq")
    pairs = [(member, (member + shift) % count) for member in range(count)]
    return lax.ppermute(block, "seq", pairs)


def fits(tile_rows, qkv_weight):
    in_rows = tile_rows.shape[0]
    seq_count, head_count = lax.axis_size("seq"), lax.axis_size("head")
    heads_here, head_dim = qkv_weight.shape[1], qkv_weight.shape[3]
    rows_here = in_rows * head_count
    total_rows = rows_here * seq_count
    segments = [total_rows // fraction for fraction in FRACTIONS]
    return (
        segments == [in_rows, rows_here, total_rows]
        and head_count == 4
        and seq_count <= 8
        and heads_here == DILATIONS[1] == DILATIONS[2] // DILATIONS[1]
        and in_rows == 4 * HALF
        and head_dim % 16 == 0
        and head_dim < HALF
    )


def fast(tile_rows, tile_route, embed_weight, norm_gain, qkv_weight, out_weight):
    seq_count = lax.axis_size("seq")
    in_rows = tile_rows.shape[0]
    width = embed_weight.shape[1]
    heads_here, head_dim = qkv_weight.shape[1], qkv_weight.shape[3]
    lead_width = LEAD * width // 3
    route = tile_route.T
    order = sorted(range(1, seq_count), key=lambda shift: -min(shift, seq_count - shift))
    lead, pick = pack(tile_rows, embed_weight, route, lead_width, seq_count)
    lead_in = [lead[0]] + [shifted(lead[shift], shift) for shift in order]
    rest, _ = pack(tile_rows, embed_weight, pick, width - lead_width, seq_count)
    rest_in = [rest[0]] + [shifted(rest[shift], shift) for shift in order]
    rest, out_weight, qkv_weight = lax.optimization_barrier((rest, out_weight, qkv_weight))
    out_over = across(out_weight, 2)
    out_pieces = [out_weight, across(out_weight, 1), out_over]
    out_pieces.append(across(out_over, 1))
    turned_weight = turn(out_pieces, False)
    by_kind = jnp.transpose(qkv_weight, (0, 2, 1, 3))
    weight = jnp.pad(by_kind, ((0, 0), (0, 0), (0, 0), (0, HALF - head_dim))).reshape(width, -1)
    lead_in, turned_weight, weight = lax.optimization_barrier((lead_in, turned_weight, weight))
    rows_lead, here = land(lead_in, in_rows)
    lead_over = across(rows_lead, 2)
    lead_beside = across(rows_lead, 1)
    lead_both = across(lead_over, 1)
    rows_rest = land_more(here, rest_in)
    rest_over = across(rows_rest, 2)
    rest_beside = across(rows_rest, 1)
    gain = norm_gain.reshape(1, width)
    sources, nears, fars = [], [], []

    def step(halves):
        qkv, far = qkv_of(halves, gain, weight, head_dim, heads_here)
        sources.append(qkv)
        nears.append(near(qkv, head_dim, heads_here))
        return far

    def spread(parts):
        far = jnp.concatenate(parts, axis=0)
        fars.extend([far] + [shifted(far, shift) for shift in order])

    far_parts = [step([rows_lead, rows_rest]), step([lead_beside, rest_beside])]
    spread(far_parts)
    turned = turn([rows_lead, rows_rest], True)
    rest_both = across(rest_over, 1)
    far_parts = [step([lead_over, rest_over]), step([lead_both, rest_both])]
    spread(far_parts)
    parts = attention_blocks(sources, fars, nears, head_dim, heads_here)
    joined = [parts[0]] + [across(parts[bit], bit) for bit in range(1, 4)]
    return finish(turned, turned_weight, joined)


LEAD = 2


def local(tile_rows, tile_route, embed_weight, norm_gain, qkv_weight, out_weight):
    run = fast if fits(tile_rows, qkv_weight) else general
    return run(tile_rows, tile_route, embed_weight, norm_gain, qkv_weight, out_weight)


def solution(mesh):
    return jax.shard_map(
        local,
        mesh=mesh,
        in_specs=(
            P(("groups", "seq", "head"), None),
            P(("groups", "seq", "head"), None),
            P(),
            P(),
            P(None, "head", None, None),
            P("head", None),
        ),
        out_specs=P(("groups", "seq", "head"), None),
        check_vma=False,
    )
```

```python
import functools

import jax
import jax.numpy as jnp
from jax import lax
from jax.experimental import pallas as pl
from jax.experimental.pallas import tpu as pltpu

from jax.sharding import PartitionSpec as P


EPSILON = 1e-05
DILATIONS = (1, 4, 16)
FRACTIONS = (16, 4, 1)


def from_partner(block, axis, apart):
    count = lax.axis_size(axis)
    route = []
    for low in range(count):
        high = low | 1 << apart
        if high != low and high < count:
            route += [(low, high), (high, low)]
    return lax.ppermute(block, axis, route)


def layer_norm(rows, gain):
    row_mean = jnp.mean(rows, axis=-1, keepdims=True)
    centered = rows - row_mean
    row_var = jnp.mean(centered * centered, axis=-1, keepdims=True)
    return (centered * lax.rsqrt(row_var + EPSILON) * gain).astype(jnp.bfloat16)


def attend_block(queries, key_rows, values):
    score_scale = queries.shape[-1] ** (-0.5)
    scores = jnp.dot(queries, key_rows.T, preferred_element_type=jnp.float32) * score_scale
    row_max = jnp.max(scores, axis=-1)
    expo = jnp.exp(scores - row_max[:, None])
    denominator = jnp.sum(expo, axis=-1)
    weights = (expo / denominator[:, None]).astype(jnp.bfloat16)
    head_out = jnp.dot(weights, values, preferred_element_type=jnp.float32)
    return (head_out, row_max + jnp.log(denominator))


def attend(queries, key_rows, values):
    count = queries.shape[0]
    if count > 512 and count % 512 == 0:
        blocks = queries.reshape(count // 512, 512, queries.shape[1])
        head_out, log_total = lax.map(
            lambda block_in: attend_block(block_in, key_rows, values), blocks
        )
        return (head_out.reshape(count, -1), log_total.reshape(count))
    return attend_block(queries, key_rows, values)


def expand_rows(head_out, log_total, offset, dilation):
    count = head_out.shape[0]
    pick_mask = jnp.arange(dilation, dtype=jnp.int32) == offset
    full_out = jnp.where(pick_mask[None, :, None], head_out[:, None, :], 0.0).reshape(
        count * dilation, -1
    )
    full_total = jnp.where(pick_mask[None, :], log_total[:, None], -1e30).reshape(count * dilation)
    return (full_out, full_total)


def merge_scales(outputs, totals):
    row_max = jnp.maximum(jnp.maximum(totals[0], totals[1]), totals[2])
    numer = jnp.zeros_like(outputs[0])
    denom = jnp.zeros_like(totals[0])
    for full_out, full_total in zip(outputs, totals):
        factor = jnp.exp(full_total - row_max)
        numer = numer + factor[:, None] * full_out
        denom = denom + factor
    return numer / denom[:, None]


def collect_segment(flat_rows, levels, seq_index):
    for level in range(levels):
        partner = from_partner(flat_rows, "seq", level)
        upper_half = seq_index >> level & 1 == 1
        lower_rows = jnp.where(upper_half, partner, flat_rows)
        upper_rows = jnp.where(upper_half, flat_rows, partner)
        flat_rows = jnp.concatenate([lower_rows, upper_rows], axis=0)
    return flat_rows


def general(tile_rows, tile_route, embed_weight, norm_gain, qkv_weight, out_weight):
    seq_count = lax.axis_size("seq")
    seq_index = lax.axis_index("seq")
    in_rows = tile_rows.shape[0]
    width = embed_weight.shape[1]
    capacity = 2 * in_rows // seq_count
    projected = jnp.dot(tile_rows, embed_weight, preferred_element_type=jnp.float32).astype(
        jnp.bfloat16
    )
    dest_seq = tile_route[:, 0]
    slot_index = tile_route[:, 1]
    owner_hits = (dest_seq[:, None] == jnp.arange(seq_count, dtype=jnp.int32)[None, :]).astype(
        jnp.int32
    )
    earlier = jnp.cumsum(owner_hits, axis=0) - owner_hits
    owner_rank = jnp.sum(earlier * owner_hits, axis=1)
    buffer_place = dest_seq * capacity + owner_rank
    send_pick = jnp.arange(seq_count * capacity, dtype=jnp.int32)[:, None] == buffer_place[None, :]
    outgoing = jnp.dot(
        send_pick.astype(jnp.bfloat16), projected, preferred_element_type=jnp.float32
    ).astype(jnp.bfloat16)
    outgoing_slot = jnp.sum(jnp.where(send_pick, slot_index[None, :] + 1, 0), axis=1)
    arrived, arrived_slot = (
        lax.all_to_all(
            outgoing.reshape(seq_count, capacity, width),
            "seq",
            split_axis=0,
            concat_axis=0,
            tiled=True,
        ),
        lax.all_to_all(
            outgoing_slot.reshape(seq_count, capacity),
            "seq",
            split_axis=0,
            concat_axis=0,
            tiled=True,
        ),
    )
    landing = jnp.arange(in_rows, dtype=jnp.int32)[:, None] + 1 == arrived_slot.reshape(-1)[None, :]
    embedded = jnp.dot(
        landing.astype(jnp.bfloat16), arrived.reshape(-1, width), preferred_element_type=jnp.float32
    )
    normed = layer_norm(embedded, norm_gain)
    heads_here = qkv_weight.shape[1]
    head_dim = qkv_weight.shape[3]
    weight_flat = qkv_weight.reshape(width, -1)
    qkv = jnp.dot(
        lax.all_gather(normed, "head", axis=0, tiled=True),
        weight_flat,
        preferred_element_type=jnp.float32,
    ).astype(jnp.bfloat16)
    rows_here = qkv.shape[0]
    qkv = qkv.reshape(rows_here, heads_here, 3, head_dim)
    first_head = lax.axis_index("head") * heads_here
    total_rows = rows_here * seq_count
    outputs = [[] for _ in range(heads_here)]
    totals = [[] for _ in range(heads_here)]
    for fraction, dilation in zip(FRACTIONS, DILATIONS):
        segment = total_rows // fraction
        per_segment = segment // dilation
        count = rows_here // dilation
        shaped = qkv.reshape(count, dilation, heads_here, 3, head_dim)
        offsets = []
        chosen = []
        for member in range(heads_here):
            offset = (first_head + member) % dilation
            offsets.append(offset)
            chosen.append(
                lax.dynamic_index_in_dim(shaped[:, :, member], offset, axis=1, keepdims=False)
            )
        chosen = jnp.stack(chosen, axis=1)
        queries = chosen[:, :, 0]
        pairs = chosen[:, :, 1:]
        if segment > rows_here:
            levels = (segment // rows_here).bit_length() - 1
            flat_rows = collect_segment(pairs.reshape(count, -1), levels, seq_index)
            pairs = flat_rows.reshape(per_segment, heads_here, 2, head_dim)
            groups = 1
        else:
            groups = rows_here // segment
        grouped_queries = queries.reshape(groups, count // groups, heads_here, head_dim)
        grouped_pairs = pairs.reshape(groups, per_segment, heads_here, 2, head_dim)
        for member in range(heads_here):
            head_out, log_total = lax.map(
                lambda block_in: attend(block_in[0], block_in[1][:, 0], block_in[1][:, 1]),
                (grouped_queries[:, :, member], grouped_pairs[:, :, member]),
            )
            full_out, full_total = expand_rows(
                head_out.reshape(count, head_dim),
                log_total.reshape(count),
                offsets[member],
                dilation,
            )
            outputs[member].append(full_out)
            totals[member].append(full_total)
    merged = [
        merge_scales(outputs[member], totals[member]).astype(jnp.bfloat16)
        for member in range(heads_here)
    ]
    attention = jnp.stack(merged, axis=1).reshape(rows_here, heads_here * head_dim)
    regrouped = lax.all_to_all(attention, "head", split_axis=0, concat_axis=1, tiled=True)
    branch = jnp.dot(
        regrouped,
        lax.all_gather(out_weight, "head", axis=0, tiled=True),
        preferred_element_type=jnp.float32,
    )
    return (embedded + branch).astype(jnp.bfloat16)


HALF = 64


def iota(shape, dim):
    return lax.broadcasted_iota(jnp.int32, shape, dim)


def matmul(left, right, dims=((1,), (0,))):
    return lax.dot_general(left, right, (dims, ((), ())), preferred_element_type=jnp.float32)


def landed_place(slot, in_rows):
    middle, last = DILATIONS[1], DILATIONS[2]
    inner = last // middle
    run = in_rows // last
    return slot % middle * (inner * run) + slot // middle % inner * run + slot // last


def pack_kernel(seq_count, rows_hbm, weight_hbm, route_ref, *refs):
    blocks = refs[:seq_count]
    picks = refs[seq_count:-3]
    rows_ref, weight_ref, arrived = refs[-3:]
    in_rows = rows_ref.shape[0]
    chunks, _, chunk = weight_ref.shape
    capacity = 2 * in_rows // seq_count
    first = weight_hbm.shape[1] - chunks * chunk if not picks else 0
    rows_copy = pltpu.make_async_copy(rows_hbm, rows_ref, arrived.at[chunks])
    rows_copy.start()
    copies = []
    for number in range(chunks):
        columns = slice(first + number * chunk, first + (number + 1) * chunk)
        copies.append(
            pltpu.make_async_copy(
                weight_hbm.at[:, columns], weight_ref.at[number], arrived.at[number]
            )
        )
        copies[number].start()

    if picks:
        me = lax.axis_index("seq")
        dest = route_ref[0:1, :]
        slot = route_ref[1:2, :]
        shift = jnp.where(dest < me, dest - me + seq_count, dest - me)
        hits = (iota((8, in_rows), 0) == shift).astype(jnp.float32)
        before = (iota((in_rows, in_rows), 0) < iota((in_rows, in_rows), 1)).astype(jnp.bfloat16)
        earlier = matmul(hits.astype(jnp.bfloat16), before)
        base = (iota((8, in_rows), 0) * capacity).astype(jnp.float32)
        place = jnp.sum(hits * (earlier + base), axis=0, keepdims=True).astype(jnp.int32)
        pick = (iota((seq_count * capacity, in_rows), 0) == place).astype(jnp.bfloat16)
        picks[0][...] = pick
        mark = (landed_place(slot, in_rows) + 1).astype(jnp.float32)
        marks = jnp.broadcast_to(mark, (8, in_rows)).astype(jnp.bfloat16)
        found = matmul(marks, pick, ((1,), (1,))).astype(jnp.bfloat16)
        for number in range(seq_count):
            spare = (blocks[number].shape[0] - capacity, blocks[number].shape[1])
            blocks[number][capacity:] = jnp.zeros(spare, jnp.bfloat16)
            blocks[number][capacity : capacity + 8, :capacity] = found[
                :, number * capacity : (number + 1) * capacity
            ]
    else:
        pick = route_ref[...]

    rows_copy.wait()
    for step in range(chunks):
        copies[step].wait()
        projected = matmul(rows_ref[...], weight_ref[step]).astype(jnp.bfloat16)
        packed = matmul(pick, projected).astype(jnp.bfloat16)
        columns = slice(step * chunk, (step + 1) * chunk)
        for number in range(seq_count):
            blocks[number][:capacity, columns] = packed[number * capacity : (number + 1) * capacity]


def pack(tile_rows, embed_weight, route, columns, seq_count):
    in_rows, depth = tile_rows.shape
    capacity = 2 * in_rows // seq_count
    chunk = 256
    lead = route.dtype == jnp.int32
    hbm = pl.BlockSpec(memory_space=pltpu.HBM)
    rows = capacity + 8 if lead else capacity
    shapes = [jax.ShapeDtypeStruct((rows, columns), jnp.bfloat16)] * seq_count
    if lead:
        shapes.append(jax.ShapeDtypeStruct((seq_count * capacity, in_rows), jnp.bfloat16))
    results = pl.pallas_call(
        functools.partial(pack_kernel, seq_count),
        in_specs=[hbm, hbm, pl.BlockSpec(memory_space=pltpu.VMEM)],
        out_shape=shapes,
        scratch_shapes=[
            pltpu.VMEM((in_rows, depth), jnp.bfloat16),
            pltpu.VMEM((columns // chunk, depth, chunk), jnp.bfloat16),
            pltpu.SemaphoreType.DMA((columns // chunk + 1,)),
        ],
        cost_estimate=cost(2 * in_rows * columns * (depth + seq_count * capacity)),
        compiler_params=pltpu.CompilerParams(vmem_limit_bytes=62 << 20),
    )(tile_rows, embed_weight, route)
    return results[:seq_count], results[-1]


LIMIT = pltpu.CompilerParams(vmem_limit_bytes=16 << 20)


def cost(flops):
    return pl.CostEstimate(flops=flops, bytes_accessed=1 << 20, transcendentals=0)


def land_kernel(count, *refs):
    blocks = refs[:count]
    rows_ref, here_ref = refs[count:]
    in_rows = rows_ref.shape[0]
    capacity = 2 * in_rows // count
    rows = jnp.zeros(rows_ref.shape, jnp.float32)
    for number, block in enumerate(blocks):
        slot = block[capacity : capacity + 8, :capacity].astype(jnp.float32)[:1]
        here = ((iota((in_rows, capacity), 0) + 1).astype(jnp.float32) == slot).astype(jnp.bfloat16)
        here_ref[:, number * capacity : (number + 1) * capacity] = here
        rows = rows + matmul(here, block[:capacity])
    rows_ref[...] = rows.astype(jnp.bfloat16)


def land(blocks, in_rows):
    count = len(blocks)
    capacity = 2 * in_rows // count
    width = blocks[0].shape[1]
    return pl.pallas_call(
        functools.partial(land_kernel, count),
        out_shape=[
            jax.ShapeDtypeStruct((in_rows, width), jnp.bfloat16),
            jax.ShapeDtypeStruct((in_rows, count * capacity), jnp.bfloat16),
        ],
        cost_estimate=cost(2 * in_rows * width * count * capacity),
        compiler_params=LIMIT,
        name="land_lead",
    )(*blocks)


def land_more_kernel(here_ref, *refs):
    blocks, rows_ref = refs[:-1], refs[-1]
    capacity = blocks[0].shape[0]
    rows = jnp.zeros(rows_ref.shape, jnp.float32)
    for number, block in enumerate(blocks):
        here = here_ref[:, number * capacity : (number + 1) * capacity]
        rows = rows + matmul(here, block[...])
    rows_ref[...] = rows.astype(jnp.bfloat16)


def land_more(here, blocks):
    in_rows, total = here.shape
    width = blocks[0].shape[1]
    return pl.pallas_call(
        land_more_kernel,
        out_shape=jax.ShapeDtypeStruct((in_rows, width), jnp.bfloat16),
        cost_estimate=cost(2 * in_rows * width * total),
        compiler_params=LIMIT,
        name="land_rest",
    )(here, *blocks)


def turn_kernel(down, *refs):
    pieces, out_ref = refs[:-1], refs[-1]
    start = 0
    for piece in pieces:
        depth = piece.shape[1 if down else 0]
        if down:
            out_ref[start : start + depth] = piece[...].T
        else:
            out_ref[:, start : start + depth] = piece[...].T
        start += depth


def turn(pieces, down):
    rows = sum(piece.shape[0] for piece in pieces)
    columns = sum(piece.shape[1] for piece in pieces)
    shape = (columns, pieces[0].shape[0]) if down else (pieces[0].shape[1], rows)
    return pl.pallas_call(
        functools.partial(turn_kernel, down),
        out_shape=jax.ShapeDtypeStruct(shape, jnp.bfloat16),
        cost_estimate=cost(len(pieces) * 100_000_000),
        compiler_params=LIMIT,
    )(*pieces)


def project_block(rows, weight, head_dim):
    out = matmul(rows, weight)
    third = out.shape[1] // 3
    lanes = iota((1, out.shape[1]), 1)
    ones = (lanes >= 2 * third) & (lanes % HALF == head_dim)
    return (out + ones.astype(jnp.float32)).astype(jnp.bfloat16)


def qkv_kernel(head_dim, heads_here, lead_ref, rest_ref, gain_ref, weight_ref, out_ref, far_ref):
    in_rows = lead_ref.shape[0]
    rows = jnp.concatenate([lead_ref[...], rest_ref[...]], axis=1).astype(jnp.float32)
    normed = layer_norm(rows, gain_ref[...])
    out_ref[...] = project_block(normed, weight_ref[...], head_dim)
    middle, last = DILATIONS[1], DILATIONS[2]
    run = in_rows // last
    third = heads_here * HALF
    inner = lax.axis_index("head") % (last // middle)
    low = iota((1, 2 * HALF), 1) < HALF
    for column in range(third, 3 * third, 2 * HALF):
        both = []
        for side in range(2):
            member = column % third // HALF + side
            row = member * (in_rows // middle) + inner * run
            both.append(out_ref[pl.ds(pl.multiple_of(row, run), run), column : column + 2 * HALF])
        far_ref[:, column - third : column - third + 2 * HALF] = jnp.where(low, both[0], both[1])


def near_kernel(head_dim, heads_here, qkv_ref, out_ref):
    in_rows = qkv_ref.shape[0]
    third = heads_here * HALF
    scale = LOG2E * head_dim ** (-0.5)
    lanes = iota((1, 2 * HALF), 1)
    for first in range(0, third, 2 * HALF):
        keys = qkv_ref[:, third + first : third + first + 2 * HALF]
        turned = qkv_ref[:, 2 * third + first : 2 * third + first + 2 * HALF].T
        for side in range(2):
            mine = (lanes // HALF == side).astype(jnp.bfloat16)
            queries = qkv_ref[:, first : first + 2 * HALF] * mine
            scores = matmul(keys, queries, ((1,), (1,)))
            values = turned[side * HALF : (side + 1) * HALF]
            total, top = softmax_product([scores], scale, [values])
            start = first + side * HALF
            out_ref[start : start + HALF] = total
            out_ref[start + HALF - 8 : start + HALF] = jnp.broadcast_to(top, (8, in_rows))


def qkv_of(halves, gain, weight, head_dim, heads_here):
    in_rows = halves[0].shape[0]
    return pl.pallas_call(
        functools.partial(qkv_kernel, head_dim, heads_here),
        out_shape=[
            jax.ShapeDtypeStruct((in_rows, weight.shape[1]), jnp.bfloat16),
            jax.ShapeDtypeStruct((in_rows // DILATIONS[2], 2 * heads_here * HALF), jnp.bfloat16),
        ],
        cost_estimate=cost(2 * in_rows * weight.shape[0] * weight.shape[1]),
        compiler_params=LIMIT,
    )(*halves, gain, weight)


def near(qkv, head_dim, heads_here):
    in_rows = qkv.shape[0]
    return pl.pallas_call(
        functools.partial(near_kernel, head_dim, heads_here),
        out_shape=jax.ShapeDtypeStruct((heads_here * HALF, in_rows), jnp.float32),
        cost_estimate=cost(heads_here * 8 * in_rows * in_rows * 128),
        compiler_params=LIMIT,
    )(qkv)


def softmax_product(scores, scale, turned):
    top = functools.reduce(jnp.maximum, [jnp.max(each, axis=0, keepdims=True) for each in scores])
    total = None
    for each, values in zip(scores, turned):
        weights = jnp.exp2(each * scale - top * scale).astype(jnp.bfloat16)
        product = matmul(values, weights)
        total = product if total is None else total + product
    return total, top


LOG2E = 1.4426950408889634


def wide_kernel(head_dim, heads_here, *refs):
    sources, fars, nears, outs = refs[:4], refs[4:-8], refs[-8:-4], refs[-4:]
    in_rows = sources[0].shape[0]
    middle, last = DILATIONS[1], DILATIONS[2]
    wide = in_rows // middle
    run = in_rows // last
    third = heads_here * HALF
    scale = LOG2E * head_dim ** (-0.5)
    inner = lax.axis_index("head") % (last // middle)
    lanes = iota((1, 2 * HALF), 1)
    chosen = iota((1, in_rows), 1) // run % (last // middle) == inner
    for pair in range(heads_here // 2):
        span = slice(pair * 2 * HALF, (pair + 1) * 2 * HALF)
        keys_at = slice(third + span.start, third + span.stop)
        values_at = slice(2 * third + span.start, 2 * third + span.stop)
        far_keys = jnp.concatenate([far[:, span] for far in fars], axis=0)
        far_turned = jnp.concatenate(
            [far[:, third + span.start : third + span.stop] for far in fars], axis=0
        ).T
        for side in range(2):
            member = 2 * pair + side
            mine = (lanes // HALF == side).astype(jnp.bfloat16)
            held = slice(side * HALF, (side + 1) * HALF)
            picked = slice(member * wide, (member + 1) * wide)

            def gathered(columns):
                return jnp.concatenate([source[picked, columns] for source in sources], axis=0)

            picked_queries = gathered(span) * mine
            middle_scores = matmul(gathered(keys_at), picked_queries, ((1,), (1,)))
            far_scores = matmul(far_keys, picked_queries, ((1,), (1,)))
            far_scores = jnp.where(chosen, far_scores, -1e30)
            wide_total, wide_top = softmax_product(
                [middle_scores, far_scores], scale, [gathered(values_at).T[held], far_turned[held]]
            )
            for number in range(4):
                base = member * HALF
                total = nears[number][base : base + HALF]
                top = nears[number][base + HALF - 8 : base + HALF][:1]
                extra, extra_top = place_lanes(wide_total, wide_top, number, member, wide)
                tile = member * wide // 128 * 128
                at = slice(tile, tile + 128)
                inside = iota((1, 128), 1) // wide == member % (128 // wide)
                extra_top = jnp.where(inside, extra_top, -1e30)
                peak = jnp.maximum(top[:, at], extra_top)
                old = jnp.exp2((top[:, at] - peak) * scale)
                new = jnp.exp2((extra_top - peak) * scale)
                merged = total[:, at] * old + jnp.where(inside, extra * new, 0.0)
                rows = slice(member * head_dim, (member + 1) * head_dim)
                for other in range(0, in_rows, 128):
                    part = merged if other == tile else total[:, other : other + 128]
                    done = part[:head_dim] / part[head_dim : head_dim + 1]
                    outs[number][rows, other : other + 128] = done.astype(jnp.bfloat16)


def place_lanes(total, top, number, member, wide):
    tile = number * wide // 128 * 128
    shift = (member * wide - number * wide) % 128
    total, top = total[:, tile : tile + 128], top[:, tile : tile + 128]
    if shift:
        total = pltpu.roll(total, shift, 1)
        top = pltpu.roll(jnp.broadcast_to(top, (8, 128)), shift, 1)[:1]
    return total, top


def attention_blocks(sources, fars, nears, head_dim, heads_here):
    in_rows = sources[0].shape[0]
    out = jax.ShapeDtypeStruct((heads_here * head_dim, in_rows), jnp.bfloat16)
    return pl.pallas_call(
        functools.partial(wide_kernel, head_dim, heads_here),
        out_shape=[out] * 4,
        cost_estimate=cost(8 * 4 * in_rows * in_rows * 128),
        compiler_params=LIMIT,
        name="wide",
    )(*sources, *fars, *nears)


def finish_kernel(turned_ref, weight_ref, *refs):
    pieces, out_ref = refs[:-1], refs[-1]
    joined = jnp.concatenate([piece[...] for piece in pieces], axis=0)
    branch = matmul(weight_ref[...], joined)
    mixed = (turned_ref[...].astype(jnp.float32) + branch).astype(jnp.bfloat16)
    in_rows = out_ref.shape[0]
    square = (in_rows, in_rows)
    back = landed_place(iota(square, 0), in_rows) == iota(square, 1)
    out_ref[...] = matmul(back.astype(jnp.bfloat16), mixed, ((1,), (1,))).astype(jnp.bfloat16)


def finish(turned, weight, pieces):
    width, in_rows = turned.shape
    return pl.pallas_call(
        finish_kernel,
        out_shape=jax.ShapeDtypeStruct((in_rows, width), jnp.bfloat16),
        cost_estimate=cost(2 * in_rows * width * (width + in_rows)),
        compiler_params=LIMIT,
        name="finish",
    )(turned, weight, *pieces)


def across(block, bit):
    count = lax.axis_size("head")
    return lax.ppermute(block, "head", [(member, member ^ bit) for member in range(count)])


def shifted(block, shift):
    count = lax.axis_size("seq")
    pairs = [(member, (member + shift) % count) for member in range(count)]
    return lax.ppermute(block, "seq", pairs)


def fits(tile_rows, qkv_weight):
    in_rows = tile_rows.shape[0]
    seq_count, head_count = lax.axis_size("seq"), lax.axis_size("head")
    heads_here, head_dim = qkv_weight.shape[1], qkv_weight.shape[3]
    rows_here = in_rows * head_count
    total_rows = rows_here * seq_count
    segments = [total_rows // fraction for fraction in FRACTIONS]
    return (
        segments == [in_rows, rows_here, total_rows]
        and head_count == 4
        and seq_count <= 8
        and heads_here == DILATIONS[1] == DILATIONS[2] // DILATIONS[1]
        and in_rows == 4 * HALF
        and head_dim % 16 == 0
        and head_dim < HALF
    )


def fast(tile_rows, tile_route, embed_weight, norm_gain, qkv_weight, out_weight):
    seq_count = lax.axis_size("seq")
    in_rows = tile_rows.shape[0]
    width = embed_weight.shape[1]
    heads_here, head_dim = qkv_weight.shape[1], qkv_weight.shape[3]
    lead_width = LEAD * width // 3
    route = tile_route.T
    order = sorted(range(1, seq_count), key=lambda shift: -min(shift, seq_count - shift))
    lead, pick = pack(tile_rows, embed_weight, route, lead_width, seq_count)
    lead_in = [lead[0]] + [shifted(lead[shift], shift) for shift in order]
    rest, _ = pack(tile_rows, embed_weight, pick, width - lead_width, seq_count)
    rest_in = [rest[0]] + [shifted(rest[shift], shift) for shift in order]
    lead_in[0], out_weight, qkv_weight = lax.optimization_barrier(
        (lead_in[0], out_weight, qkv_weight)
    )
    out_over = across(out_weight, 2)
    out_pieces = [out_weight, across(out_weight, 1), out_over]
    out_pieces.append(across(out_over, 1))
    turned_weight = turn(out_pieces, False)
    by_kind = jnp.transpose(qkv_weight, (0, 2, 1, 3))
    weight = jnp.pad(by_kind, ((0, 0), (0, 0), (0, 0), (0, HALF - head_dim))).reshape(width, -1)
    lead_in, weight = lax.optimization_barrier((lead_in, weight))
    rows_lead, here = land(lead_in, in_rows)
    lead_over = across(rows_lead, 2)
    lead_beside = across(rows_lead, 1)
    lead_both = across(lead_over, 1)
    rows_rest = land_more(here, rest_in)
    rest_over = across(rows_rest, 2)
    rest_beside = across(rows_rest, 1)
    gain = norm_gain.reshape(1, width)
    sources, nears, far_parts = [], [], []

    def step(halves):
        qkv, far = qkv_of(halves, gain, weight, head_dim, heads_here)
        sources.append(qkv)
        nears.append(near(qkv, head_dim, heads_here))
        far_parts.append(far)

    step([rows_lead, rows_rest])
    step([lead_beside, rest_beside])
    turned = turn([rows_lead, rows_rest], True)
    rest_both = across(rest_over, 1)
    step([lead_over, rest_over])
    step([lead_both, rest_both])
    far = jnp.concatenate(far_parts, axis=0)
    fars = [far] + [shifted(far, shift) for shift in order]
    parts = attention_blocks(sources, fars, nears, head_dim, heads_here)
    joined = [parts[0]] + [across(parts[bit], bit) for bit in range(1, 4)]
    return finish(turned, turned_weight, joined)


LEAD = 2


def local(tile_rows, tile_route, embed_weight, norm_gain, qkv_weight, out_weight):
    run = fast if fits(tile_rows, qkv_weight) else general
    return run(tile_rows, tile_route, embed_weight, norm_gain, qkv_weight, out_weight)


def solution(mesh):
    return jax.shard_map(
        local,
        mesh=mesh,
        in_specs=(
            P(("groups", "seq", "head"), None),
            P(("groups", "seq", "head"), None),
            P(),
            P(),
            P(None, "head", None, None),
            P("head", None),
        ),
        out_specs=P(("groups", "seq", "head"), None),
        check_vma=False,
    )
```

```python
import functools

import jax
import jax.numpy as jnp
from jax import lax
from jax.experimental import pallas as pl
from jax.experimental.pallas import tpu as pltpu

from jax.sharding import PartitionSpec as P


EPSILON = 1e-05
DILATIONS = (1, 4, 16)
FRACTIONS = (16, 4, 1)


def from_partner(block, axis, apart):
    count = lax.axis_size(axis)
    route = []
    for low in range(count):
        high = low | 1 << apart
        if high != low and high < count:
            route += [(low, high), (high, low)]
    return lax.ppermute(block, axis, route)


def layer_norm(rows, gain):
    row_mean = jnp.mean(rows, axis=-1, keepdims=True)
    centered = rows - row_mean
    row_var = jnp.mean(centered * centered, axis=-1, keepdims=True)
    return (centered * lax.rsqrt(row_var + EPSILON) * gain).astype(jnp.bfloat16)


def attend_block(queries, key_rows, values):
    score_scale = queries.shape[-1] ** (-0.5)
    scores = jnp.dot(queries, key_rows.T, preferred_element_type=jnp.float32) * score_scale
    row_max = jnp.max(scores, axis=-1)
    expo = jnp.exp(scores - row_max[:, None])
    denominator = jnp.sum(expo, axis=-1)
    weights = (expo / denominator[:, None]).astype(jnp.bfloat16)
    head_out = jnp.dot(weights, values, preferred_element_type=jnp.float32)
    return (head_out, row_max + jnp.log(denominator))


def attend(queries, key_rows, values):
    count = queries.shape[0]
    if count > 512 and count % 512 == 0:
        blocks = queries.reshape(count // 512, 512, queries.shape[1])
        head_out, log_total = lax.map(
            lambda block_in: attend_block(block_in, key_rows, values), blocks
        )
        return (head_out.reshape(count, -1), log_total.reshape(count))
    return attend_block(queries, key_rows, values)


def expand_rows(head_out, log_total, offset, dilation):
    count = head_out.shape[0]
    pick_mask = jnp.arange(dilation, dtype=jnp.int32) == offset
    full_out = jnp.where(pick_mask[None, :, None], head_out[:, None, :], 0.0).reshape(
        count * dilation, -1
    )
    full_total = jnp.where(pick_mask[None, :], log_total[:, None], -1e30).reshape(count * dilation)
    return (full_out, full_total)


def merge_scales(outputs, totals):
    row_max = jnp.maximum(jnp.maximum(totals[0], totals[1]), totals[2])
    numer = jnp.zeros_like(outputs[0])
    denom = jnp.zeros_like(totals[0])
    for full_out, full_total in zip(outputs, totals):
        factor = jnp.exp(full_total - row_max)
        numer = numer + factor[:, None] * full_out
        denom = denom + factor
    return numer / denom[:, None]


def collect_segment(flat_rows, levels, seq_index):
    for level in range(levels):
        partner = from_partner(flat_rows, "seq", level)
        upper_half = seq_index >> level & 1 == 1
        lower_rows = jnp.where(upper_half, partner, flat_rows)
        upper_rows = jnp.where(upper_half, flat_rows, partner)
        flat_rows = jnp.concatenate([lower_rows, upper_rows], axis=0)
    return flat_rows


def general(tile_rows, tile_route, embed_weight, norm_gain, qkv_weight, out_weight):
    seq_count = lax.axis_size("seq")
    seq_index = lax.axis_index("seq")
    in_rows = tile_rows.shape[0]
    width = embed_weight.shape[1]
    capacity = 2 * in_rows // seq_count
    projected = jnp.dot(tile_rows, embed_weight, preferred_element_type=jnp.float32).astype(
        jnp.bfloat16
    )
    dest_seq = tile_route[:, 0]
    slot_index = tile_route[:, 1]
    owner_hits = (dest_seq[:, None] == jnp.arange(seq_count, dtype=jnp.int32)[None, :]).astype(
        jnp.int32
    )
    earlier = jnp.cumsum(owner_hits, axis=0) - owner_hits
    owner_rank = jnp.sum(earlier * owner_hits, axis=1)
    buffer_place = dest_seq * capacity + owner_rank
    send_pick = jnp.arange(seq_count * capacity, dtype=jnp.int32)[:, None] == buffer_place[None, :]
    outgoing = jnp.dot(
        send_pick.astype(jnp.bfloat16), projected, preferred_element_type=jnp.float32
    ).astype(jnp.bfloat16)
    outgoing_slot = jnp.sum(jnp.where(send_pick, slot_index[None, :] + 1, 0), axis=1)
    arrived, arrived_slot = (
        lax.all_to_all(
            outgoing.reshape(seq_count, capacity, width),
            "seq",
            split_axis=0,
            concat_axis=0,
            tiled=True,
        ),
        lax.all_to_all(
            outgoing_slot.reshape(seq_count, capacity),
            "seq",
            split_axis=0,
            concat_axis=0,
            tiled=True,
        ),
    )
    landing = jnp.arange(in_rows, dtype=jnp.int32)[:, None] + 1 == arrived_slot.reshape(-1)[None, :]
    embedded = jnp.dot(
        landing.astype(jnp.bfloat16), arrived.reshape(-1, width), preferred_element_type=jnp.float32
    )
    normed = layer_norm(embedded, norm_gain)
    heads_here = qkv_weight.shape[1]
    head_dim = qkv_weight.shape[3]
    weight_flat = qkv_weight.reshape(width, -1)
    qkv = jnp.dot(
        lax.all_gather(normed, "head", axis=0, tiled=True),
        weight_flat,
        preferred_element_type=jnp.float32,
    ).astype(jnp.bfloat16)
    rows_here = qkv.shape[0]
    qkv = qkv.reshape(rows_here, heads_here, 3, head_dim)
    first_head = lax.axis_index("head") * heads_here
    total_rows = rows_here * seq_count
    outputs = [[] for _ in range(heads_here)]
    totals = [[] for _ in range(heads_here)]
    for fraction, dilation in zip(FRACTIONS, DILATIONS):
        segment = total_rows // fraction
        per_segment = segment // dilation
        count = rows_here // dilation
        shaped = qkv.reshape(count, dilation, heads_here, 3, head_dim)
        offsets = []
        chosen = []
        for member in range(heads_here):
            offset = (first_head + member) % dilation
            offsets.append(offset)
            chosen.append(
                lax.dynamic_index_in_dim(shaped[:, :, member], offset, axis=1, keepdims=False)
            )
        chosen = jnp.stack(chosen, axis=1)
        queries = chosen[:, :, 0]
        pairs = chosen[:, :, 1:]
        if segment > rows_here:
            levels = (segment // rows_here).bit_length() - 1
            flat_rows = collect_segment(pairs.reshape(count, -1), levels, seq_index)
            pairs = flat_rows.reshape(per_segment, heads_here, 2, head_dim)
            groups = 1
        else:
            groups = rows_here // segment
        grouped_queries = queries.reshape(groups, count // groups, heads_here, head_dim)
        grouped_pairs = pairs.reshape(groups, per_segment, heads_here, 2, head_dim)
        for member in range(heads_here):
            head_out, log_total = lax.map(
                lambda block_in: attend(block_in[0], block_in[1][:, 0], block_in[1][:, 1]),
                (grouped_queries[:, :, member], grouped_pairs[:, :, member]),
            )
            full_out, full_total = expand_rows(
                head_out.reshape(count, head_dim),
                log_total.reshape(count),
                offsets[member],
                dilation,
            )
            outputs[member].append(full_out)
            totals[member].append(full_total)
    merged = [
        merge_scales(outputs[member], totals[member]).astype(jnp.bfloat16)
        for member in range(heads_here)
    ]
    attention = jnp.stack(merged, axis=1).reshape(rows_here, heads_here * head_dim)
    regrouped = lax.all_to_all(attention, "head", split_axis=0, concat_axis=1, tiled=True)
    branch = jnp.dot(
        regrouped,
        lax.all_gather(out_weight, "head", axis=0, tiled=True),
        preferred_element_type=jnp.float32,
    )
    return (embedded + branch).astype(jnp.bfloat16)


HALF = 64


def iota(shape, dim):
    return lax.broadcasted_iota(jnp.int32, shape, dim)


def matmul(left, right, dims=((1,), (0,))):
    return lax.dot_general(left, right, (dims, ((), ())), preferred_element_type=jnp.float32)


def landed_place(slot, in_rows):
    middle, last = DILATIONS[1], DILATIONS[2]
    inner = last // middle
    run = in_rows // last
    return slot % middle * (inner * run) + slot // middle % inner * run + slot // last


def slot_of(place, in_rows):
    middle, last = DILATIONS[1], DILATIONS[2]
    inner = last // middle
    run = in_rows // last
    return place % run * last + place // run % inner * middle + place // (inner * run)


def pack_kernel(seq_count, rows_hbm, weight_hbm, route_ref, *refs):
    blocks = refs[:seq_count]
    picks = refs[seq_count:-3]
    rows_ref, weight_ref, arrived = refs[-3:]
    in_rows = rows_ref.shape[1]
    parts, depth, columns = weight_ref.shape
    capacity = 2 * in_rows // seq_count
    first = 0 if picks else weight_hbm.shape[1] - columns
    copies = []
    for part in range(parts):
        span = slice(part * depth, (part + 1) * depth)
        copies.append(
            (
                pltpu.make_async_copy(rows_hbm.at[:, span], rows_ref.at[part], arrived.at[2 * part]),
                pltpu.make_async_copy(
                    weight_hbm.at[span, first : first + columns],
                    weight_ref.at[part],
                    arrived.at[2 * part + 1],
                ),
            )
        )
        for copy in copies[part]:
            copy.start()

    if picks:
        me = lax.axis_index("seq")
        dest = route_ref[0:1, :]
        slot = route_ref[1:2, :]
        shift = dest ^ me
        hits = (iota((8, in_rows), 0) == shift).astype(jnp.float32)
        before = (iota((in_rows, in_rows), 0) < iota((in_rows, in_rows), 1)).astype(jnp.bfloat16)
        earlier = matmul(hits.astype(jnp.bfloat16), before)
        base = (iota((8, in_rows), 0) * capacity).astype(jnp.float32)
        place = jnp.sum(hits * (earlier + base), axis=0, keepdims=True).astype(jnp.int32)
        pick = (iota((seq_count * capacity, in_rows), 0) == place).astype(jnp.bfloat16)
        picks[0][...] = pick
        mark = (landed_place(slot, in_rows) + 1).astype(jnp.float32)
        marks = jnp.broadcast_to(mark, (8, in_rows)).astype(jnp.bfloat16)
        found = matmul(marks, pick, ((1,), (1,))).astype(jnp.bfloat16)
        for number in range(seq_count):
            spare = (blocks[number].shape[0] - capacity, blocks[number].shape[1])
            blocks[number][capacity:] = jnp.zeros(spare, jnp.bfloat16)
            blocks[number][capacity : capacity + 8, :capacity] = found[
                :, number * capacity : (number + 1) * capacity
            ]
    else:
        pick = route_ref[...]

    projected = None
    for part in range(parts):
        for copy in copies[part]:
            copy.wait()
        product = matmul(rows_ref[part], weight_ref[part])
        projected = product if projected is None else projected + product
    packed = matmul(pick, projected.astype(jnp.bfloat16)).astype(jnp.bfloat16)
    for number in range(seq_count):
        blocks[number][:capacity] = packed[number * capacity : (number + 1) * capacity]


def pack(tile_rows, embed_weight, route, columns, seq_count):
    in_rows, depth = tile_rows.shape
    capacity = 2 * in_rows // seq_count
    parts = PARTS
    lead = route.dtype == jnp.int32
    hbm = pl.BlockSpec(memory_space=pltpu.HBM)
    rows = capacity + 8 if lead else capacity
    shapes = [jax.ShapeDtypeStruct((rows, columns), jnp.bfloat16)] * seq_count
    if lead:
        shapes.append(jax.ShapeDtypeStruct((seq_count * capacity, in_rows), jnp.bfloat16))
    results = pl.pallas_call(
        functools.partial(pack_kernel, seq_count),
        in_specs=[hbm, hbm, pl.BlockSpec(memory_space=pltpu.VMEM)],
        out_shape=shapes,
        scratch_shapes=[
            pltpu.VMEM((parts, in_rows, depth // parts), jnp.bfloat16),
            pltpu.VMEM((parts, depth // parts, columns), jnp.bfloat16),
            pltpu.SemaphoreType.DMA((2 * parts,)),
        ],
        cost_estimate=cost(2 * in_rows * columns * (depth + seq_count * capacity)),
        compiler_params=pltpu.CompilerParams(vmem_limit_bytes=62 << 20),
    )(tile_rows, embed_weight, route)
    return results[:seq_count], results[-1]


LIMIT = pltpu.CompilerParams(vmem_limit_bytes=16 << 20)


def cost(flops):
    return pl.CostEstimate(flops=flops, bytes_accessed=1 << 20, transcendentals=0)


def land_kernel(count, *refs):
    blocks = refs[:count]
    rows_ref, here_ref = refs[count:]
    in_rows = rows_ref.shape[0]
    capacity = 2 * in_rows // count
    rows = jnp.zeros(rows_ref.shape, jnp.float32)
    for number, block in enumerate(blocks):
        slot = block[capacity : capacity + 8, :capacity].astype(jnp.float32)[:1]
        here = ((iota((in_rows, capacity), 0) + 1).astype(jnp.float32) == slot).astype(jnp.bfloat16)
        here_ref[:, number * capacity : (number + 1) * capacity] = here
        rows = rows + matmul(here, block[:capacity])
    rows_ref[...] = rows.astype(jnp.bfloat16)


def land(blocks, in_rows):
    count = len(blocks)
    capacity = 2 * in_rows // count
    width = blocks[0].shape[1]
    return pl.pallas_call(
        functools.partial(land_kernel, count),
        out_shape=[
            jax.ShapeDtypeStruct((in_rows, width), jnp.bfloat16),
            jax.ShapeDtypeStruct((in_rows, count * capacity), jnp.bfloat16),
        ],
        cost_estimate=cost(2 * in_rows * width * count * capacity),
        compiler_params=LIMIT,
        name="land_lead",
    )(*blocks)


def land_more_kernel(here_ref, *refs):
    blocks, rows_ref = refs[:-1], refs[-1]
    capacity = blocks[0].shape[0]
    rows = jnp.zeros(rows_ref.shape, jnp.float32)
    for number, block in enumerate(blocks):
        here = here_ref[:, number * capacity : (number + 1) * capacity]
        rows = rows + matmul(here, block[...])
    rows_ref[...] = rows.astype(jnp.bfloat16)


def land_more(here, blocks):
    in_rows, total = here.shape
    width = blocks[0].shape[1]
    return pl.pallas_call(
        land_more_kernel,
        out_shape=jax.ShapeDtypeStruct((in_rows, width), jnp.bfloat16),
        cost_estimate=cost(2 * in_rows * width * total),
        compiler_params=LIMIT,
        name="land_rest",
    )(here, *blocks)


def turn_kernel(down, *refs):
    pieces, out_ref = refs[:-1], refs[-1]
    start = 0
    for piece in pieces:
        depth = piece.shape[1 if down else 0]
        if down:
            out_ref[start : start + depth] = piece[...].T
        else:
            out_ref[:, start : start + depth] = piece[...].T
        start += depth


def turn(pieces, down):
    rows = sum(piece.shape[0] for piece in pieces)
    columns = sum(piece.shape[1] for piece in pieces)
    shape = (columns, pieces[0].shape[0]) if down else (pieces[0].shape[1], rows)
    return pl.pallas_call(
        functools.partial(turn_kernel, down),
        out_shape=jax.ShapeDtypeStruct(shape, jnp.bfloat16),
        cost_estimate=cost(len(pieces) * 100_000_000),
        compiler_params=LIMIT,
    )(*pieces)


def project_block(rows, weight, head_dim):
    out = matmul(rows, weight, ((1,), (1,)))
    third = out.shape[1] // 3
    lanes = iota((1, out.shape[1]), 1)
    ones = (lanes >= 2 * third) & (lanes % HALF == head_dim)
    return (out + ones.astype(jnp.float32)).astype(jnp.bfloat16)


def qkv_kernel(head_dim, heads_here, lead_ref, rest_ref, gain_ref, weight_ref, out_ref, far_ref):
    in_rows = lead_ref.shape[0]
    rows = jnp.concatenate([lead_ref[...], rest_ref[...]], axis=1).astype(jnp.float32)
    normed = layer_norm(rows, gain_ref[...])
    out_ref[...] = project_block(normed, weight_ref[...], head_dim)
    middle, last = DILATIONS[1], DILATIONS[2]
    run = in_rows // last
    third = heads_here * HALF
    inner = lax.axis_index("head") % (last // middle)
    pieces = []
    for part in (1, 2):
        for member in range(heads_here):
            row = member * (in_rows // middle) + inner * run
            tile = part * third + member // 2 * 2 * HALF
            held = out_ref[pl.ds(pl.multiple_of(row, run), run), tile : tile + 2 * HALF]
            start = member % 2 * HALF
            pieces.append(held[:, start : start + head_dim])
    far_ref[...] = jnp.concatenate(pieces, axis=1)


def near_kernel(head_dim, heads_here, qkv_ref, out_ref):
    in_rows = qkv_ref.shape[0]
    third = heads_here * HALF
    scale = LOG2E * head_dim ** (-0.5)
    lanes = iota((1, 2 * HALF), 1)
    for first in range(0, third, 2 * HALF):
        keys = qkv_ref[:, third + first : third + first + 2 * HALF]
        turned = qkv_ref[:, 2 * third + first : 2 * third + first + 2 * HALF].T
        for side in range(2):
            mine = (lanes // HALF == side).astype(jnp.bfloat16)
            queries = qkv_ref[:, first : first + 2 * HALF] * mine
            scores = matmul(keys, queries, ((1,), (1,)))
            values = turned[side * HALF : (side + 1) * HALF]
            total, top = softmax_product([scores], scale, [values])
            start = first + side * HALF
            out_ref[start : start + HALF] = total
            out_ref[start + HALF - 8 : start + HALF] = jnp.broadcast_to(top, (8, in_rows))


def qkv_of(halves, gain, weight, head_dim, heads_here):
    in_rows = halves[0].shape[0]
    return pl.pallas_call(
        functools.partial(qkv_kernel, head_dim, heads_here),
        out_shape=[
            jax.ShapeDtypeStruct((in_rows, weight.shape[0]), jnp.bfloat16),
            jax.ShapeDtypeStruct((in_rows // DILATIONS[2], 2 * heads_here * head_dim), jnp.bfloat16),
        ],
        cost_estimate=cost(2 * in_rows * weight.shape[0] * weight.shape[1]),
        compiler_params=LIMIT,
    )(*halves, gain, weight)


def near(qkv, head_dim, heads_here):
    in_rows = qkv.shape[0]
    return pl.pallas_call(
        functools.partial(near_kernel, head_dim, heads_here),
        out_shape=jax.ShapeDtypeStruct((heads_here * HALF, in_rows), jnp.float32),
        cost_estimate=cost(heads_here * 8 * in_rows * in_rows * 128),
        compiler_params=LIMIT,
    )(qkv)


def softmax_product(scores, scale, turned):
    top = functools.reduce(jnp.maximum, [jnp.max(each, axis=0, keepdims=True) for each in scores])
    total = None
    for each, values in zip(scores, turned):
        weights = jnp.exp2(each * scale - top * scale).astype(jnp.bfloat16)
        product = matmul(values, weights)
        total = product if total is None else total + product
    return total, top


LOG2E = 1.4426950408889634


def middle_kernel(head_dim, heads_here, *refs):
    sources, out_ref = refs[:-1], refs[-1]
    wide_rows = sources[0].shape[0] // DILATIONS[1]
    third = heads_here * HALF
    scale = LOG2E * head_dim ** (-0.5)
    lanes = iota((1, 2 * HALF), 1)
    for member in range(heads_here):
        picked = slice(member * wide_rows, (member + 1) * wide_rows)
        tile = member // 2 * 2 * HALF
        side = member % 2

        def gathered(part):
            start = part * third + tile
            return jnp.concatenate(
                [source[picked, start : start + 2 * HALF] for source in sources], axis=0
            )

        queries = gathered(0) * (lanes // HALF == side).astype(jnp.bfloat16)
        scores = matmul(gathered(1), queries, ((1,), (1,)))
        values = gathered(2).T[side * HALF : (side + 1) * HALF]
        total, top = softmax_product([scores], scale, [values])
        start = member * HALF
        out_ref[start : start + HALF] = total
        out_ref[start + HALF - 8 : start + HALF] = jnp.broadcast_to(top, (8, total.shape[1]))


def middle_of(sources, head_dim, heads_here):
    lanes = len(sources) * sources[0].shape[0] // DILATIONS[1]
    return pl.pallas_call(
        functools.partial(middle_kernel, head_dim, heads_here),
        out_shape=jax.ShapeDtypeStruct((heads_here * HALF, lanes), jnp.float32),
        cost_estimate=cost(heads_here * 8 * lanes * lanes * 128),
        compiler_params=LIMIT,
        name="middle",
    )(*sources)


def joined_totals(first, first_top, second, second_top, scale):
    peak = jnp.maximum(first_top, second_top)
    first_weight = jnp.exp2((first_top - peak) * scale)
    second_weight = jnp.exp2((second_top - peak) * scale)
    return first * first_weight + second * second_weight, peak


def wide_kernel(head_dim, heads_here, numbers, middle_ref, *refs):
    count = len(numbers)
    sources, fars = refs[:count], refs[count : -2 * count]
    nears, outs = refs[-2 * count : -count], refs[-count:]
    in_rows = sources[0].shape[0]
    middle, last = DILATIONS[1], DILATIONS[2]
    wide = in_rows // middle
    run = in_rows // last
    scale = LOG2E * head_dim ** (-0.5)
    inner = lax.axis_index("head") % (last // middle)
    chosen = iota((1, count * wide), 1) // run % (last // middle) == inner
    lanes_at = slice(numbers[0] * wide, (numbers[0] + count) * wide)
    far_rows = jnp.concatenate([far[...] for far in fars], axis=0)
    sums = (iota((HALF - head_dim, far_rows.shape[0]), 0) == 0).astype(jnp.bfloat16)
    for member in range(heads_here):
        base = member * HALF
        picked = slice(member * wide, (member + 1) * wide)
        tile = member // 2 * 2 * HALF
        start = member % 2 * HALF
        queries = jnp.concatenate(
            [source[picked, tile : tile + 2 * HALF] for source in sources], axis=0
        )[:, start : start + head_dim]
        keys = far_rows[:, member * head_dim : (member + 1) * head_dim]
        first = (heads_here + member) * head_dim
        values = jnp.concatenate([far_rows[:, first : first + head_dim].T, sums], axis=0)
        scores = jnp.where(chosen, matmul(keys, queries, ((1,), (1,))), -1e30)
        far_total, far_top = softmax_product([scores], scale, [values])
        wide_total, wide_top = joined_totals(
            middle_ref[base : base + HALF, lanes_at],
            middle_ref[base + HALF - 8 : base + HALF, lanes_at][:1],
            far_total,
            far_top,
            scale,
        )
        for number in range(count):
            total = nears[number][base : base + HALF]
            top = nears[number][base + HALF - 8 : base + HALF][:1]
            extra, extra_top = place_lanes(wide_total, wide_top, number, member, wide)
            tile = member * wide // 128 * 128
            at = slice(tile, tile + 128)
            inside = iota((1, 128), 1) // wide == member % (128 // wide)
            extra_top = jnp.where(inside, extra_top, -1e30)
            peak = jnp.maximum(top[:, at], extra_top)
            old = jnp.exp2((top[:, at] - peak) * scale)
            new = jnp.exp2((extra_top - peak) * scale)
            merged = total[:, at] * old + jnp.where(inside, extra * new, 0.0)
            rows = slice(member * head_dim, (member + 1) * head_dim)
            for other in range(0, in_rows, 128):
                part = merged if other == tile else total[:, other : other + 128]
                done = part[:head_dim] / part[head_dim : head_dim + 1]
                outs[number][rows, other : other + 128] = done.astype(jnp.bfloat16)


def place_lanes(total, top, number, member, wide):
    tile = number * wide // 128 * 128
    shift = (member * wide - number * wide) % 128
    total, top = total[:, tile : tile + 128], top[:, tile : tile + 128]
    if shift:
        total = pltpu.roll(total, shift, 1)
        top = pltpu.roll(jnp.broadcast_to(top, (8, 128)), shift, 1)[:1]
    return total, top


def wide(middle, sources, fars, nears, numbers, head_dim, heads_here):
    in_rows = sources[0].shape[0]
    out = jax.ShapeDtypeStruct((heads_here * head_dim, in_rows), jnp.bfloat16)
    return pl.pallas_call(
        functools.partial(wide_kernel, head_dim, heads_here, numbers),
        out_shape=[out] * len(numbers),
        cost_estimate=cost(4 * 4 * in_rows * in_rows * 128),
        compiler_params=LIMIT,
    )(
        middle,
        *[sources[number] for number in numbers],
        *fars,
        *[nears[number] for number in numbers],
    )


def start_kernel(turned_ref, weight_ref, *refs):
    pieces, out_ref = refs[:-1], refs[-1]
    joined = jnp.concatenate([piece[...] for piece in pieces], axis=0)
    out_ref[...] = turned_ref[...].astype(jnp.float32) + matmul(weight_ref[...], joined)


def finish_kernel(begun_ref, weight_ref, *refs):
    pieces, out_ref = refs[:-1], refs[-1]
    joined = jnp.concatenate([piece[...] for piece in pieces], axis=0)
    mixed = (begun_ref[...] + matmul(weight_ref[...], joined)).astype(jnp.bfloat16)
    in_rows = out_ref.shape[0]
    back = iota((in_rows, in_rows), 0) == slot_of(iota((1, in_rows), 1), in_rows)
    out_ref[...] = matmul(back.astype(jnp.bfloat16), mixed, ((1,), (1,))).astype(jnp.bfloat16)


def with_pieces(kernel, begun, weight, pieces, shape):
    width, in_rows = begun.shape
    return pl.pallas_call(
        kernel,
        out_shape=shape,
        cost_estimate=cost(2 * in_rows * width * (width + in_rows)),
        compiler_params=LIMIT,
    )(begun, weight, *pieces)


def across(block, bit):
    count = lax.axis_size("head")
    return lax.ppermute(block, "head", [(member, member ^ bit) for member in range(count)])


def shifted(block, shift):
    count = lax.axis_size("seq")
    pairs = [(member, member ^ shift) for member in range(count)]
    return lax.ppermute(block, "seq", pairs)


def fits(tile_rows, qkv_weight):
    in_rows = tile_rows.shape[0]
    seq_count, head_count = lax.axis_size("seq"), lax.axis_size("head")
    heads_here, head_dim = qkv_weight.shape[1], qkv_weight.shape[3]
    rows_here = in_rows * head_count
    total_rows = rows_here * seq_count
    segments = [total_rows // fraction for fraction in FRACTIONS]
    return (
        segments == [in_rows, rows_here, total_rows]
        and head_count == 4
        and seq_count == 4
        and heads_here == DILATIONS[1] == DILATIONS[2] // DILATIONS[1]
        and in_rows == 4 * HALF
        and head_dim % 16 == 0
        and head_dim < HALF
    )


def fast(tile_rows, tile_route, embed_weight, norm_gain, qkv_weight, out_weight):
    seq_count = lax.axis_size("seq")
    in_rows = tile_rows.shape[0]
    width = embed_weight.shape[1]
    heads_here, head_dim = qkv_weight.shape[1], qkv_weight.shape[3]
    lead_width = width // 2
    route = tile_route.T
    order = sorted(range(1, seq_count), key=lambda shift: shift < seq_count // 2)
    lead, pick = pack(tile_rows, embed_weight, route, lead_width, seq_count)
    lead_in = [lead[0]] + [shifted(lead[shift], shift) for shift in order]
    rest, _ = pack(tile_rows, embed_weight, pick, width - lead_width, seq_count)
    rest_in = [rest[0]] + [shifted(rest[shift], shift) for shift in order]
    lead_in[0], out_weight, qkv_weight = lax.optimization_barrier(
        (lead_in[0], out_weight, qkv_weight)
    )
    out_over = across(out_weight, 2)
    out_pieces = [out_weight, across(out_weight, 1), out_over]
    out_pieces.append(across(out_over, 1))
    turned_here = turn(out_pieces[:2], False)
    turned_there = turn(out_pieces[2:], False)
    by_kind = jnp.transpose(qkv_weight, (2, 1, 3, 0))
    weight = jnp.pad(by_kind, ((0, 0), (0, 0), (0, HALF - head_dim), (0, 0))).reshape(-1, width)
    lead_in, weight = lax.optimization_barrier((lead_in, weight))
    rows_lead, here = land(lead_in, in_rows)
    lead_over = across(rows_lead, 2)
    lead_beside = across(rows_lead, 1)
    lead_both = across(lead_over, 1)
    rows_rest = land_more(here, rest_in)
    rest_over = across(rows_rest, 2)
    rest_beside = across(rows_rest, 1)
    gain = norm_gain.reshape(1, width)
    sources, nears, far_parts = [], [], []

    def step(halves):
        qkv, far = qkv_of(halves, gain, weight, head_dim, heads_here)
        sources.append(qkv)
        nears.append(near(qkv, head_dim, heads_here))
        far_parts.append(far)

    step([rows_lead, rows_rest])
    step([lead_beside, rest_beside])
    turned = turn([rows_lead, rows_rest], True)
    rest_both = across(rest_over, 1)
    step([lead_over, rest_over])
    step([lead_both, rest_both])
    far = jnp.concatenate(far_parts, axis=0)
    fars = [far] + [shifted(far, shift) for shift in order]
    middle = middle_of(sources, head_dim, heads_here)
    there = wide(middle, sources, fars, nears, (2, 3), head_dim, heads_here)
    here = wide(middle, sources, fars, nears, (0, 1), head_dim, heads_here)
    near_pieces = [here[0], across(here[1], 1)]
    far_pieces = [across(there[0], 2), across(there[1], 3)]
    shape = jax.ShapeDtypeStruct(turned.shape, jnp.float32)
    begun = with_pieces(start_kernel, turned, turned_here, near_pieces, shape)
    shape = jax.ShapeDtypeStruct((in_rows, width), jnp.bfloat16)
    return with_pieces(finish_kernel, begun, turned_there, far_pieces, shape)


PARTS = 2


def local(tile_rows, tile_route, embed_weight, norm_gain, qkv_weight, out_weight):
    run = fast if fits(tile_rows, qkv_weight) else general
    return run(tile_rows, tile_route, embed_weight, norm_gain, qkv_weight, out_weight)


def solution(mesh):
    return jax.shard_map(
        local,
        mesh=mesh,
        in_specs=(
            P(("groups", "seq", "head"), None),
            P(("groups", "seq", "head"), None),
            P(),
            P(),
            P(None, "head", None, None),
            P("head", None),
        ),
        out_specs=P(("groups", "seq", "head"), None),
        check_vma=False,
    )
```

```python
import functools

import jax
import jax.numpy as jnp
from jax import lax
from jax.experimental import pallas as pl
from jax.experimental.pallas import tpu as pltpu

from jax.sharding import PartitionSpec as P


EPSILON = 1e-05
DILATIONS = (1, 4, 16)
FRACTIONS = (16, 4, 1)


def from_partner(block, axis, apart):
    count = lax.axis_size(axis)
    route = []
    for low in range(count):
        high = low | 1 << apart
        if high != low and high < count:
            route += [(low, high), (high, low)]
    return lax.ppermute(block, axis, route)


def layer_norm(rows, gain):
    row_mean = jnp.mean(rows, axis=-1, keepdims=True)
    centered = rows - row_mean
    row_var = jnp.mean(centered * centered, axis=-1, keepdims=True)
    return (centered * lax.rsqrt(row_var + EPSILON) * gain).astype(jnp.bfloat16)


def attend_block(queries, key_rows, values):
    score_scale = queries.shape[-1] ** (-0.5)
    scores = jnp.dot(queries, key_rows.T, preferred_element_type=jnp.float32) * score_scale
    row_max = jnp.max(scores, axis=-1)
    expo = jnp.exp(scores - row_max[:, None])
    denominator = jnp.sum(expo, axis=-1)
    weights = (expo / denominator[:, None]).astype(jnp.bfloat16)
    head_out = jnp.dot(weights, values, preferred_element_type=jnp.float32)
    return (head_out, row_max + jnp.log(denominator))


def attend(queries, key_rows, values):
    count = queries.shape[0]
    if count > 512 and count % 512 == 0:
        blocks = queries.reshape(count // 512, 512, queries.shape[1])
        head_out, log_total = lax.map(
            lambda block_in: attend_block(block_in, key_rows, values), blocks
        )
        return (head_out.reshape(count, -1), log_total.reshape(count))
    return attend_block(queries, key_rows, values)


def expand_rows(head_out, log_total, offset, dilation):
    count = head_out.shape[0]
    pick_mask = jnp.arange(dilation, dtype=jnp.int32) == offset
    full_out = jnp.where(pick_mask[None, :, None], head_out[:, None, :], 0.0).reshape(
        count * dilation, -1
    )
    full_total = jnp.where(pick_mask[None, :], log_total[:, None], -1e30).reshape(count * dilation)
    return (full_out, full_total)


def merge_scales(outputs, totals):
    row_max = jnp.maximum(jnp.maximum(totals[0], totals[1]), totals[2])
    numer = jnp.zeros_like(outputs[0])
    denom = jnp.zeros_like(totals[0])
    for full_out, full_total in zip(outputs, totals):
        factor = jnp.exp(full_total - row_max)
        numer = numer + factor[:, None] * full_out
        denom = denom + factor
    return numer / denom[:, None]


def collect_segment(flat_rows, levels, seq_index):
    for level in range(levels):
        partner = from_partner(flat_rows, "seq", level)
        upper_half = seq_index >> level & 1 == 1
        lower_rows = jnp.where(upper_half, partner, flat_rows)
        upper_rows = jnp.where(upper_half, flat_rows, partner)
        flat_rows = jnp.concatenate([lower_rows, upper_rows], axis=0)
    return flat_rows


def general(tile_rows, tile_route, embed_weight, norm_gain, qkv_weight, out_weight):
    seq_count = lax.axis_size("seq")
    seq_index = lax.axis_index("seq")
    in_rows = tile_rows.shape[0]
    width = embed_weight.shape[1]
    capacity = 2 * in_rows // seq_count
    projected = jnp.dot(tile_rows, embed_weight, preferred_element_type=jnp.float32).astype(
        jnp.bfloat16
    )
    dest_seq = tile_route[:, 0]
    slot_index = tile_route[:, 1]
    owner_hits = (dest_seq[:, None] == jnp.arange(seq_count, dtype=jnp.int32)[None, :]).astype(
        jnp.int32
    )
    earlier = jnp.cumsum(owner_hits, axis=0) - owner_hits
    owner_rank = jnp.sum(earlier * owner_hits, axis=1)
    buffer_place = dest_seq * capacity + owner_rank
    send_pick = jnp.arange(seq_count * capacity, dtype=jnp.int32)[:, None] == buffer_place[None, :]
    outgoing = jnp.dot(
        send_pick.astype(jnp.bfloat16), projected, preferred_element_type=jnp.float32
    ).astype(jnp.bfloat16)
    outgoing_slot = jnp.sum(jnp.where(send_pick, slot_index[None, :] + 1, 0), axis=1)
    arrived, arrived_slot = (
        lax.all_to_all(
            outgoing.reshape(seq_count, capacity, width),
            "seq",
            split_axis=0,
            concat_axis=0,
            tiled=True,
        ),
        lax.all_to_all(
            outgoing_slot.reshape(seq_count, capacity),
            "seq",
            split_axis=0,
            concat_axis=0,
            tiled=True,
        ),
    )
    landing = jnp.arange(in_rows, dtype=jnp.int32)[:, None] + 1 == arrived_slot.reshape(-1)[None, :]
    embedded = jnp.dot(
        landing.astype(jnp.bfloat16), arrived.reshape(-1, width), preferred_element_type=jnp.float32
    )
    normed = layer_norm(embedded, norm_gain)
    heads_here = qkv_weight.shape[1]
    head_dim = qkv_weight.shape[3]
    weight_flat = qkv_weight.reshape(width, -1)
    qkv = jnp.dot(
        lax.all_gather(normed, "head", axis=0, tiled=True),
        weight_flat,
        preferred_element_type=jnp.float32,
    ).astype(jnp.bfloat16)
    rows_here = qkv.shape[0]
    qkv = qkv.reshape(rows_here, heads_here, 3, head_dim)
    first_head = lax.axis_index("head") * heads_here
    total_rows = rows_here * seq_count
    outputs = [[] for _ in range(heads_here)]
    totals = [[] for _ in range(heads_here)]
    for fraction, dilation in zip(FRACTIONS, DILATIONS):
        segment = total_rows // fraction
        per_segment = segment // dilation
        count = rows_here // dilation
        shaped = qkv.reshape(count, dilation, heads_here, 3, head_dim)
        offsets = []
        chosen = []
        for member in range(heads_here):
            offset = (first_head + member) % dilation
            offsets.append(offset)
            chosen.append(
                lax.dynamic_index_in_dim(shaped[:, :, member], offset, axis=1, keepdims=False)
            )
        chosen = jnp.stack(chosen, axis=1)
        queries = chosen[:, :, 0]
        pairs = chosen[:, :, 1:]
        if segment > rows_here:
            levels = (segment // rows_here).bit_length() - 1
            flat_rows = collect_segment(pairs.reshape(count, -1), levels, seq_index)
            pairs = flat_rows.reshape(per_segment, heads_here, 2, head_dim)
            groups = 1
        else:
            groups = rows_here // segment
        grouped_queries = queries.reshape(groups, count // groups, heads_here, head_dim)
        grouped_pairs = pairs.reshape(groups, per_segment, heads_here, 2, head_dim)
        for member in range(heads_here):
            head_out, log_total = lax.map(
                lambda block_in: attend(block_in[0], block_in[1][:, 0], block_in[1][:, 1]),
                (grouped_queries[:, :, member], grouped_pairs[:, :, member]),
            )
            full_out, full_total = expand_rows(
                head_out.reshape(count, head_dim),
                log_total.reshape(count),
                offsets[member],
                dilation,
            )
            outputs[member].append(full_out)
            totals[member].append(full_total)
    merged = [
        merge_scales(outputs[member], totals[member]).astype(jnp.bfloat16)
        for member in range(heads_here)
    ]
    attention = jnp.stack(merged, axis=1).reshape(rows_here, heads_here * head_dim)
    regrouped = lax.all_to_all(attention, "head", split_axis=0, concat_axis=1, tiled=True)
    branch = jnp.dot(
        regrouped,
        lax.all_gather(out_weight, "head", axis=0, tiled=True),
        preferred_element_type=jnp.float32,
    )
    return (embedded + branch).astype(jnp.bfloat16)


HALF = 64


def iota(shape, dim):
    return lax.broadcasted_iota(jnp.int32, shape, dim)


def matmul(left, right, dims=((1,), (0,))):
    return lax.dot_general(left, right, (dims, ((), ())), preferred_element_type=jnp.float32)


def landed_place(slot, in_rows):
    middle, last = DILATIONS[1], DILATIONS[2]
    inner = last // middle
    run = in_rows // last
    return slot % middle * (inner * run) + slot // middle % inner * run + slot // last


def slot_of(place, in_rows):
    middle, last = DILATIONS[1], DILATIONS[2]
    inner = last // middle
    run = in_rows // last
    return place % run * last + place // run % inner * middle + place // (inner * run)


def pack_kernel(seq_count, rows_hbm, weight_hbm, route_ref, *refs):
    blocks = refs[:seq_count]
    picks = refs[seq_count:-3]
    rows_ref, weight_ref, arrived = refs[-3:]
    in_rows = rows_ref.shape[1]
    parts, depth, columns = weight_ref.shape
    capacity = 2 * in_rows // seq_count
    first = 0 if picks else weight_hbm.shape[1] - columns
    copies = []
    for part in range(parts):
        span = slice(part * depth, (part + 1) * depth)
        copies.append(
            (
                pltpu.make_async_copy(rows_hbm.at[:, span], rows_ref.at[part], arrived.at[2 * part]),
                pltpu.make_async_copy(
                    weight_hbm.at[span, first : first + columns],
                    weight_ref.at[part],
                    arrived.at[2 * part + 1],
                ),
            )
        )
        for copy in copies[part]:
            copy.start()

    if picks:
        me = lax.axis_index("seq")
        dest = route_ref[0:1, :]
        slot = route_ref[1:2, :]
        shift = dest ^ me
        hits = (iota((8, in_rows), 0) == shift).astype(jnp.float32)
        before = (iota((in_rows, in_rows), 0) < iota((in_rows, in_rows), 1)).astype(jnp.bfloat16)
        earlier = matmul(hits.astype(jnp.bfloat16), before)
        base = (iota((8, in_rows), 0) * capacity).astype(jnp.float32)
        place = jnp.sum(hits * (earlier + base), axis=0, keepdims=True).astype(jnp.int32)
        pick = (iota((seq_count * capacity, in_rows), 0) == place).astype(jnp.bfloat16)
        picks[0][...] = pick
        mark = (landed_place(slot, in_rows) + 1).astype(jnp.float32)
        marks = jnp.broadcast_to(mark, (8, in_rows)).astype(jnp.bfloat16)
        found = matmul(marks, pick, ((1,), (1,))).astype(jnp.bfloat16)
        for number in range(seq_count):
            spare = (blocks[number].shape[0] - capacity, blocks[number].shape[1])
            blocks[number][capacity:] = jnp.zeros(spare, jnp.bfloat16)
            blocks[number][capacity : capacity + 8, :capacity] = found[
                :, number * capacity : (number + 1) * capacity
            ]
    else:
        pick = route_ref[...]

    projected = None
    for part in range(parts):
        for copy in copies[part]:
            copy.wait()
        product = matmul(rows_ref[part], weight_ref[part])
        projected = product if projected is None else projected + product
    packed = matmul(pick, projected.astype(jnp.bfloat16)).astype(jnp.bfloat16)
    for number in range(seq_count):
        blocks[number][:capacity] = packed[number * capacity : (number + 1) * capacity]


def pack(tile_rows, embed_weight, route, columns, seq_count):
    in_rows, depth = tile_rows.shape
    capacity = 2 * in_rows // seq_count
    parts = PARTS
    lead = route.dtype == jnp.int32
    hbm = pl.BlockSpec(memory_space=pltpu.HBM)
    rows = capacity + 8 if lead else capacity
    shapes = [jax.ShapeDtypeStruct((rows, columns), jnp.bfloat16)] * seq_count
    if lead:
        shapes.append(jax.ShapeDtypeStruct((seq_count * capacity, in_rows), jnp.bfloat16))
    results = pl.pallas_call(
        functools.partial(pack_kernel, seq_count),
        in_specs=[hbm, hbm, pl.BlockSpec(memory_space=pltpu.VMEM)],
        out_shape=shapes,
        scratch_shapes=[
            pltpu.VMEM((parts, in_rows, depth // parts), jnp.bfloat16),
            pltpu.VMEM((parts, depth // parts, columns), jnp.bfloat16),
            pltpu.SemaphoreType.DMA((2 * parts,)),
        ],
        cost_estimate=cost(2 * in_rows * columns * (depth + seq_count * capacity)),
        compiler_params=pltpu.CompilerParams(vmem_limit_bytes=54000 << 10),
    )(tile_rows, embed_weight, route)
    return results[:seq_count], results[-1]


LIMIT = pltpu.CompilerParams(vmem_limit_bytes=16 << 20)


def cost(flops):
    return pl.CostEstimate(flops=flops, bytes_accessed=1 << 20, transcendentals=0)


def land_kernel(count, *refs):
    blocks = refs[:count]
    rows_ref, here_ref = refs[count:]
    in_rows = rows_ref.shape[0]
    capacity = 2 * in_rows // count
    rows = jnp.zeros(rows_ref.shape, jnp.float32)
    for number, block in enumerate(blocks):
        slot = block[capacity : capacity + 8, :capacity].astype(jnp.float32)[:1]
        here = ((iota((in_rows, capacity), 0) + 1).astype(jnp.float32) == slot).astype(jnp.bfloat16)
        here_ref[:, number * capacity : (number + 1) * capacity] = here
        rows = rows + matmul(here, block[:capacity])
    rows_ref[...] = rows.astype(jnp.bfloat16)


def land(blocks, in_rows):
    count = len(blocks)
    capacity = 2 * in_rows // count
    width = blocks[0].shape[1]
    return pl.pallas_call(
        functools.partial(land_kernel, count),
        out_shape=[
            jax.ShapeDtypeStruct((in_rows, width), jnp.bfloat16),
            jax.ShapeDtypeStruct((in_rows, count * capacity), jnp.bfloat16),
        ],
        cost_estimate=cost(2 * in_rows * width * count * capacity),
        compiler_params=LIMIT,
        name="land_lead",
    )(*blocks)


def land_more_kernel(here_ref, *refs):
    blocks, rows_ref = refs[:-1], refs[-1]
    capacity = blocks[0].shape[0]
    rows = jnp.zeros(rows_ref.shape, jnp.float32)
    for number, block in enumerate(blocks):
        here = here_ref[:, number * capacity : (number + 1) * capacity]
        rows = rows + matmul(here, block[...])
    rows_ref[...] = rows.astype(jnp.bfloat16)


def land_more(here, blocks):
    in_rows, total = here.shape
    width = blocks[0].shape[1]
    return pl.pallas_call(
        land_more_kernel,
        out_shape=jax.ShapeDtypeStruct((in_rows, width), jnp.bfloat16),
        cost_estimate=cost(2 * in_rows * width * total),
        compiler_params=LIMIT,
        name="land_rest",
    )(here, *blocks)


def turn_kernel(down, *refs):
    pieces, out_ref = refs[:-1], refs[-1]
    start = 0
    for piece in pieces:
        depth = piece.shape[1 if down else 0]
        if down:
            out_ref[start : start + depth] = piece[...].T
        else:
            out_ref[:, start : start + depth] = piece[...].T
        start += depth


def turn(pieces, down):
    rows = sum(piece.shape[0] for piece in pieces)
    columns = sum(piece.shape[1] for piece in pieces)
    shape = (columns, pieces[0].shape[0]) if down else (pieces[0].shape[1], rows)
    return pl.pallas_call(
        functools.partial(turn_kernel, down),
        out_shape=jax.ShapeDtypeStruct(shape, jnp.bfloat16),
        cost_estimate=cost(len(pieces) * 100_000_000),
        compiler_params=LIMIT,
    )(*pieces)


def project_block(rows, weight, head_dim):
    out = matmul(rows, weight, ((1,), (1,)))
    third = out.shape[1] // 3
    lanes = iota((1, out.shape[1]), 1)
    ones = (lanes >= 2 * third) & (lanes % HALF == head_dim)
    return (out + ones.astype(jnp.float32)).astype(jnp.bfloat16)


def qkv_kernel(head_dim, heads_here, lead_ref, rest_ref, gain_ref, weight_ref, out_ref, far_ref):
    in_rows = lead_ref.shape[0]
    rows = jnp.concatenate([lead_ref[...], rest_ref[...]], axis=1).astype(jnp.float32)
    normed = layer_norm(rows, gain_ref[...])
    out_ref[...] = project_block(normed, weight_ref[...], head_dim)
    middle, last = DILATIONS[1], DILATIONS[2]
    run = in_rows // last
    third = heads_here * HALF
    inner = lax.axis_index("head") % (last // middle)
    pieces = []
    for part in (1, 2):
        for member in range(heads_here):
            row = member * (in_rows // middle) + inner * run
            tile = part * third + member // 2 * 2 * HALF
            held = out_ref[pl.ds(pl.multiple_of(row, run), run), tile : tile + 2 * HALF]
            start = member % 2 * HALF
            pieces.append(held[:, start : start + head_dim])
    far_ref[...] = jnp.concatenate(pieces, axis=1)


def near_kernel(head_dim, heads_here, qkv_ref, out_ref):
    in_rows = qkv_ref.shape[0]
    third = heads_here * HALF
    scale = LOG2E * head_dim ** (-0.5)
    lanes = iota((1, 2 * HALF), 1)
    for first in range(0, third, 2 * HALF):
        keys = qkv_ref[:, third + first : third + first + 2 * HALF]
        turned = qkv_ref[:, 2 * third + first : 2 * third + first + 2 * HALF].T
        for side in range(2):
            mine = (lanes // HALF == side).astype(jnp.bfloat16)
            queries = qkv_ref[:, first : first + 2 * HALF] * mine
            scores = matmul(keys, queries, ((1,), (1,)))
            values = turned[side * HALF : (side + 1) * HALF]
            total, top = softmax_product([scores], scale, [values])
            start = first + side * HALF
            out_ref[start : start + HALF] = total
            out_ref[start + HALF - 8 : start + HALF] = jnp.broadcast_to(top, (8, in_rows))


def qkv_of(halves, gain, weight, head_dim, heads_here):
    in_rows = halves[0].shape[0]
    return pl.pallas_call(
        functools.partial(qkv_kernel, head_dim, heads_here),
        out_shape=[
            jax.ShapeDtypeStruct((in_rows, weight.shape[0]), jnp.bfloat16),
            jax.ShapeDtypeStruct((in_rows // DILATIONS[2], 2 * heads_here * head_dim), jnp.bfloat16),
        ],
        cost_estimate=cost(2 * in_rows * weight.shape[0] * weight.shape[1]),
        compiler_params=LIMIT,
    )(*halves, gain, weight)


def near(qkv, head_dim, heads_here):
    in_rows = qkv.shape[0]
    return pl.pallas_call(
        functools.partial(near_kernel, head_dim, heads_here),
        out_shape=jax.ShapeDtypeStruct((heads_here * HALF, in_rows), jnp.float32),
        cost_estimate=cost(heads_here * 8 * in_rows * in_rows * 128),
        compiler_params=LIMIT,
    )(qkv)


def softmax_product(scores, scale, turned):
    top = functools.reduce(jnp.maximum, [jnp.max(each, axis=0, keepdims=True) for each in scores])
    total = None
    for each, values in zip(scores, turned):
        weights = jnp.exp2(each * scale - top * scale).astype(jnp.bfloat16)
        product = matmul(values, weights)
        total = product if total is None else total + product
    return total, top


LOG2E = 1.4426950408889634


def middle_kernel(head_dim, heads_here, *refs):
    sources, out_ref = refs[:-1], refs[-1]
    wide_rows = sources[0].shape[0] // DILATIONS[1]
    third = heads_here * HALF
    scale = LOG2E * head_dim ** (-0.5)
    lanes = iota((1, 2 * HALF), 1)
    for member in range(heads_here):
        picked = slice(member * wide_rows, (member + 1) * wide_rows)
        tile = member // 2 * 2 * HALF
        side = member % 2

        def gathered(part):
            start = part * third + tile
            return jnp.concatenate(
                [source[picked, start : start + 2 * HALF] for source in sources], axis=0
            )

        queries = gathered(0) * (lanes // HALF == side).astype(jnp.bfloat16)
        scores = matmul(gathered(1), queries, ((1,), (1,)))
        values = gathered(2).T[side * HALF : (side + 1) * HALF]
        total, top = softmax_product([scores], scale, [values])
        start = member * HALF
        out_ref[start : start + HALF] = total
        out_ref[start + HALF - 8 : start + HALF] = jnp.broadcast_to(top, (8, total.shape[1]))


def middle_of(sources, head_dim, heads_here):
    lanes = len(sources) * sources[0].shape[0] // DILATIONS[1]
    return pl.pallas_call(
        functools.partial(middle_kernel, head_dim, heads_here),
        out_shape=jax.ShapeDtypeStruct((heads_here * HALF, lanes), jnp.float32),
        cost_estimate=cost(heads_here * 8 * lanes * lanes * 128),
        compiler_params=LIMIT,
        name="middle",
    )(*sources)


def joined_totals(first, first_top, second, second_top, scale):
    peak = jnp.maximum(first_top, second_top)
    first_weight = jnp.exp2((first_top - peak) * scale)
    second_weight = jnp.exp2((second_top - peak) * scale)
    return first * first_weight + second * second_weight, peak


def wide_kernel(head_dim, heads_here, numbers, middle_ref, *refs):
    count = len(numbers)
    sources, fars = refs[:count], refs[count : -2 * count]
    nears, outs = refs[-2 * count : -count], refs[-count:]
    in_rows = sources[0].shape[0]
    middle, last = DILATIONS[1], DILATIONS[2]
    wide = in_rows // middle
    run = in_rows // last
    scale = LOG2E * head_dim ** (-0.5)
    inner = lax.axis_index("head") % (last // middle)
    chosen = iota((1, count * wide), 1) // run % (last // middle) == inner
    lanes_at = slice(numbers[0] * wide, (numbers[0] + count) * wide)
    far_rows = jnp.concatenate([far[...] for far in fars], axis=0)
    sums = (iota((HALF - head_dim, far_rows.shape[0]), 0) == 0).astype(jnp.bfloat16)
    for member in range(heads_here):
        base = member * HALF
        picked = slice(member * wide, (member + 1) * wide)
        tile = member // 2 * 2 * HALF
        start = member % 2 * HALF
        queries = jnp.concatenate(
            [source[picked, tile : tile + 2 * HALF] for source in sources], axis=0
        )[:, start : start + head_dim]
        keys = far_rows[:, member * head_dim : (member + 1) * head_dim]
        first = (heads_here + member) * head_dim
        values = jnp.concatenate([far_rows[:, first : first + head_dim].T, sums], axis=0)
        scores = jnp.where(chosen, matmul(keys, queries, ((1,), (1,))), -1e30)
        far_total, far_top = softmax_product([scores], scale, [values])
        wide_total, wide_top = joined_totals(
            middle_ref[base : base + HALF, lanes_at],
            middle_ref[base + HALF - 8 : base + HALF, lanes_at][:1],
            far_total,
            far_top,
            scale,
        )
        for number in range(count):
            total = nears[number][base : base + HALF]
            top = nears[number][base + HALF - 8 : base + HALF][:1]
            extra, extra_top = place_lanes(wide_total, wide_top, number, member, wide)
            tile = member * wide // 128 * 128
            at = slice(tile, tile + 128)
            inside = iota((1, 128), 1) // wide == member % (128 // wide)
            extra_top = jnp.where(inside, extra_top, -1e30)
            peak = jnp.maximum(top[:, at], extra_top)
            old = jnp.exp2((top[:, at] - peak) * scale)
            new = jnp.exp2((extra_top - peak) * scale)
            merged = total[:, at] * old + jnp.where(inside, extra * new, 0.0)
            rows = slice(member * head_dim, (member + 1) * head_dim)
            for other in range(0, in_rows, 128):
                part = merged if other == tile else total[:, other : other + 128]
                done = part[:head_dim] / part[head_dim : head_dim + 1]
                outs[number][rows, other : other + 128] = done.astype(jnp.bfloat16)


def place_lanes(total, top, number, member, wide):
    tile = number * wide // 128 * 128
    shift = (member * wide - number * wide) % 128
    total, top = total[:, tile : tile + 128], top[:, tile : tile + 128]
    if shift:
        total = pltpu.roll(total, shift, 1)
        top = pltpu.roll(jnp.broadcast_to(top, (8, 128)), shift, 1)[:1]
    return total, top


def wide(middle, sources, fars, nears, numbers, head_dim, heads_here):
    in_rows = sources[0].shape[0]
    out = jax.ShapeDtypeStruct((heads_here * head_dim, in_rows), jnp.bfloat16)
    return pl.pallas_call(
        functools.partial(wide_kernel, head_dim, heads_here, numbers),
        out_shape=[out] * len(numbers),
        cost_estimate=cost(4 * 4 * in_rows * in_rows * 128),
        compiler_params=LIMIT,
    )(
        middle,
        *[sources[number] for number in numbers],
        *fars,
        *[nears[number] for number in numbers],
    )


def start_kernel(turned_ref, weight_ref, *refs):
    pieces, out_ref = refs[:-1], refs[-1]
    joined = jnp.concatenate([piece[...] for piece in pieces], axis=0)
    out_ref[...] = turned_ref[...].astype(jnp.float32) + matmul(weight_ref[...], joined)


def finish_kernel(begun_ref, weight_ref, *refs):
    pieces, out_ref = refs[:-1], refs[-1]
    joined = jnp.concatenate([piece[...] for piece in pieces], axis=0)
    mixed = (begun_ref[...] + matmul(weight_ref[...], joined)).astype(jnp.bfloat16)
    in_rows = out_ref.shape[0]
    back = iota((in_rows, in_rows), 0) == slot_of(iota((1, in_rows), 1), in_rows)
    out_ref[...] = matmul(back.astype(jnp.bfloat16), mixed, ((1,), (1,))).astype(jnp.bfloat16)


def with_pieces(kernel, begun, weight, pieces, shape):
    width, in_rows = begun.shape
    return pl.pallas_call(
        kernel,
        out_shape=shape,
        cost_estimate=cost(2 * in_rows * width * (width + in_rows)),
        compiler_params=LIMIT,
    )(begun, weight, *pieces)


def across(block, bit):
    count = lax.axis_size("head")
    return lax.ppermute(block, "head", [(member, member ^ bit) for member in range(count)])


def shifted(block, shift):
    count = lax.axis_size("seq")
    pairs = [(member, member ^ shift) for member in range(count)]
    return lax.ppermute(block, "seq", pairs)


def fits(tile_rows, qkv_weight):
    in_rows = tile_rows.shape[0]
    seq_count, head_count = lax.axis_size("seq"), lax.axis_size("head")
    heads_here, head_dim = qkv_weight.shape[1], qkv_weight.shape[3]
    rows_here = in_rows * head_count
    total_rows = rows_here * seq_count
    segments = [total_rows // fraction for fraction in FRACTIONS]
    return (
        segments == [in_rows, rows_here, total_rows]
        and head_count == 4
        and seq_count == 4
        and heads_here == DILATIONS[1] == DILATIONS[2] // DILATIONS[1]
        and in_rows == 4 * HALF
        and head_dim % 16 == 0
        and head_dim < HALF
    )


def fast(tile_rows, tile_route, embed_weight, norm_gain, qkv_weight, out_weight):
    seq_count = lax.axis_size("seq")
    in_rows = tile_rows.shape[0]
    width = embed_weight.shape[1]
    heads_here, head_dim = qkv_weight.shape[1], qkv_weight.shape[3]
    lead_width = width // 2
    route = tile_route.T
    order = sorted(range(1, seq_count), key=lambda shift: shift < seq_count // 2)
    lead, pick = pack(tile_rows, embed_weight, route, lead_width, seq_count)
    lead_in = [lead[0]] + [shifted(lead[shift], shift) for shift in order]
    rest, _ = pack(tile_rows, embed_weight, pick, width - lead_width, seq_count)
    rest_in = [rest[0]] + [shifted(rest[shift], shift) for shift in order]
    lead_in[0], out_weight, qkv_weight = lax.optimization_barrier(
        (lead_in[0], out_weight, qkv_weight)
    )
    out_over = across(out_weight, 2)
    out_pieces = [out_weight, across(out_weight, 1), out_over]
    out_pieces.append(across(out_over, 1))
    turned_here = turn(out_pieces[:2], False)
    turned_there = turn(out_pieces[2:], False)
    by_kind = jnp.transpose(qkv_weight, (2, 1, 3, 0))
    weight = jnp.pad(by_kind, ((0, 0), (0, 0), (0, HALF - head_dim), (0, 0))).reshape(-1, width)
    lead_in, weight = lax.optimization_barrier((lead_in, weight))
    rows_lead, here = land(lead_in, in_rows)
    lead_over = across(rows_lead, 2)
    lead_beside = across(rows_lead, 1)
    lead_both = across(lead_over, 1)
    rows_rest = land_more(here, rest_in)
    rest_over = across(rows_rest, 2)
    rest_beside = across(rows_rest, 1)
    gain = norm_gain.reshape(1, width)
    sources, nears, far_parts = [], [], []

    def step(halves):
        qkv, far = qkv_of(halves, gain, weight, head_dim, heads_here)
        sources.append(qkv)
        nears.append(near(qkv, head_dim, heads_here))
        far_parts.append(far)

    step([rows_lead, rows_rest])
    step([lead_beside, rest_beside])
    turned = turn([rows_lead, rows_rest], True)
    rest_both = across(rest_over, 1)
    step([lead_over, rest_over])
    step([lead_both, rest_both])
    far = jnp.concatenate(far_parts, axis=0)
    fars = [far] + [shifted(far, shift) for shift in (3, 2, 1)]
    middle = middle_of(sources, head_dim, heads_here)
    there = wide(middle, sources, fars, nears, (2, 3), head_dim, heads_here)
    here = wide(middle, sources, fars, nears, (0, 1), head_dim, heads_here)
    near_pieces = [here[0], across(here[1], 1)]
    far_pieces = [across(there[0], 2), across(there[1], 3)]
    shape = jax.ShapeDtypeStruct(turned.shape, jnp.float32)
    begun = with_pieces(start_kernel, turned, turned_here, near_pieces, shape)
    shape = jax.ShapeDtypeStruct((in_rows, width), jnp.bfloat16)
    return with_pieces(finish_kernel, begun, turned_there, far_pieces, shape)


PARTS = 3


def local(tile_rows, tile_route, embed_weight, norm_gain, qkv_weight, out_weight):
    run = fast if fits(tile_rows, qkv_weight) else general
    return run(tile_rows, tile_route, embed_weight, norm_gain, qkv_weight, out_weight)


def solution(mesh):
    return jax.shard_map(
        local,
        mesh=mesh,
        in_specs=(
            P(("groups", "seq", "head"), None),
            P(("groups", "seq", "head"), None),
            P(),
            P(),
            P(None, "head", None, None),
            P("head", None),
        ),
        out_specs=P(("groups", "seq", "head"), None),
        check_vma=False,
    )
```
